32 devices in a mesh: gx: 16 (over z, y, x), gz: 2 (over core).
Axes of the slice: x: 2, y: 2, z: 4, core: 2. Of those that a mesh axis runs over, the one named last changes fastest.
Arguments:
- state: float32 [5, 128, 16, 256], P(None, 'gx', None, 'gz'), may hold values from -1 to 8.5, as said below
- register: float32 [5, 128, 16, 256], P(None, 'gx', None, 'gz'), may hold values from -2.4 to 2.4
- top_ghost: float32 [5, 128, 3, 256], P(None, 'gx', None, 'gz'), may hold values from -1 to 8.5, as said below
- flags: int32 [128, 16, 2], P('gx', None, 'gz'), may hold values 0 or 1
Outputs:
- new_state: float32 [5, 128, 16, 256], P(None, 'gx', None, 'gz')
- new_register: float32 [5, 128, 16, 256], P(None, 'gx', None, 'gz')
The draws below stay inside these ranges and needn't reach their ends.
Inputs may be any that keep to these rules, and one draw needn't show every extreme that they name: `state`: conserved variables of an ideal gas with ratio of heats 1.4, density 0.5 to 2 and pressure 0.3 to 1.5 in every cell. `top_ghost`: conserved variables of an ideal gas with ratio of heats 1.4, density 0.5 to 2 and pressure 0.3 to 1.5 in every cell.
All inputs are finite; a program needn't handle non-finite values. No bound on the sum of `flags` on one device may be relied on, other than what follows from the above.
Results may differ from the reference program's by a relative error of at most 0.0003.
Values sent between devices are 32-bit elements; how exact they have to be, the bound alone decides.
A program may use at most 64 MiB of HBM per device.

```python
import math
import jax
import jax.numpy as jnp
from jax import lax

CX = 8
NY = 16
CZ = 128
ZBLOCK = 128
NX = 128
NZ = 256
N_GX = 16


def speed_levels(key):
    keys = jax.random.split(jax.random.fold_in(key, 31), 2)
    stream_count = NX // CX
    span_count = NZ // CZ
    base = jax.random.uniform(keys[0], (stream_count,), jnp.float32, 0.0, 1.0)
    stream_level = 0.6 + 0.4 * base * base * base * base
    span_level = jax.random.uniform(keys[1], (span_count,), jnp.float32, 0.6, 1.0)
    stream_cells = jnp.repeat(stream_level, CX, total_repeat_length=NX)
    span_cells = jnp.repeat(span_level, CZ, total_repeat_length=NZ)
    return stream_cells[:, None, None] * span_cells[None, None, :]


def gas_state(key, shape, level):
    keys = jax.random.split(key, 5)
    density = jnp.exp(jax.random.uniform(keys[0], shape, jnp.float32, math.log(0.5), math.log(2.0)))
    vel_x = jax.random.uniform(keys[1], shape, jnp.float32, 0.4, 2.0)
    vel_y = jax.random.uniform(keys[2], shape, jnp.float32, -0.5, 0.5)
    vel_z = jax.random.uniform(keys[3], shape, jnp.float32, -0.5, 0.5)
    pressure = jnp.exp(jax.random.uniform(keys[4], shape, jnp.float32, math.log(0.3), math.log(1.5)))
    vel_x = vel_x * level
    vel_y = vel_y * level
    vel_z = vel_z * level
    energy = pressure / 0.4 + 0.5 * density * (vel_x * vel_x + vel_y * vel_y + vel_z * vel_z)
    return jnp.stack([density, density * vel_x, density * vel_y, density * vel_z, energy])


def draw_state(key, part):
    return gas_state(jax.random.fold_in(key, 11), (NX, NY, NZ), speed_levels(key))


def draw_top_ghost(key, part):
    return gas_state(jax.random.fold_in(key, 23), (NX, 3, NZ), speed_levels(key))


def set_ends(result, key, low, largest):
    shape = result.shape
    spot = [jax.random.randint(jax.random.fold_in(key, axis), (), 0, shape[axis]) for axis in range(len(shape))]
    result = result.at[tuple(spot)].set(low)
    longest = shape.index(max(shape))
    spot[longest] = (spot[longest] + 1) % shape[longest]
    return result.at[tuple(spot)].set(largest)


def level_of(stream_key, dims, cuts, smallest, top_value):
    loudness, own = 1.0, jax.random.fold_in(stream_key, 6)
    for dim, blocks in cuts:
        heights = jnp.exp(jax.random.uniform(jax.random.fold_in(own, dim), (blocks,), jnp.float32, smallest / len(cuts), top_value / len(cuts)))
        loudness = loudness * jnp.repeat(heights, dims[dim] // blocks).reshape([-1 if axis == dim else 1 for axis in range(len(dims))])
    return loudness


def normal_values(key, extent, spread, reach, cuts=(), kind=jnp.bfloat16):
    factor_of = level_of(key, extent, cuts, -0.22, 0.18) if cuts else 1.0
    result = jax.random.normal(key, extent, jnp.float32) * spread * factor_of
    return jnp.minimum(jnp.maximum(result, -reach), reach).astype(kind)


def setup_inputs(seed: int = 0) -> dict:
    streams_of = jax.random.split(jax.random.key(seed), 5)
    return {
        "state": draw_state(jax.random.fold_in(streams_of[4], 71), 0),
        "register": normal_values(streams_of[1], (5, NX, NY, NZ), 0.4, 2.4, ((1, 16), (3, 2)), jnp.float32),
        "top_ghost": draw_top_ghost(jax.random.fold_in(streams_of[4], 71), 0),
        "flags": set_ends((jax.random.randint(streams_of[3], (NX, NY, NZ // ZBLOCK), 0, 2) < 1).astype(jnp.int32), jax.random.fold_in(streams_of[3], 1), 0, 1),
    }


GAMMA = 1.4
EPS_WENO = 1e-06
LAMBDA_X = 0.1
LAMBDA_Y = 0.15
LAMBDA_Z = 0.1
REGISTER_DECAY = -5.0 / 9.0
UPDATE_WEIGHT = 15.0 / 16.0

def primitives(cons):
    density = cons[0]
    inverse = 1.0 / density
    vel_x = cons[1] * inverse
    vel_y = cons[2] * inverse
    vel_z = cons[3] * inverse
    pressure = (GAMMA - 1.0) * (cons[4] - 0.5 * (cons[1] * vel_x + cons[2] * vel_y + cons[3] * vel_z))
    return (density, vel_x, vel_y, vel_z, pressure)

def local_speeds(prims):
    density, vel_x, vel_y, vel_z, pressure = prims
    sound = jnp.sqrt(GAMMA * pressure / density)
    return jnp.stack([jnp.max(jnp.abs(vel_x) + sound), jnp.max(jnp.abs(vel_y) + sound), jnp.max(jnp.abs(vel_z) + sound)])

def physical_flux(cons, prims, var):
    pressure = prims[4]
    velocity = prims[var]
    rows = [cons[0] * velocity, cons[1] * velocity, cons[2] * velocity, cons[3] * velocity, (cons[4] + pressure) * velocity]
    rows[var] = rows[var] + pressure
    return jnp.stack(rows)

def weno_face(vals):
    first, second, third, fourth, fifth = vals
    cand_a = (2.0 * first - 7.0 * second + 11.0 * third) / 6.0
    cand_b = (-second + 5.0 * third + 2.0 * fourth) / 6.0
    cand_c = (2.0 * third + 5.0 * fourth - fifth) / 6.0
    smooth_a = 13.0 / 12.0 * (first - 2.0 * second + third) ** 2 + 0.25 * (first - 4.0 * second + 3.0 * third) ** 2
    smooth_b = 13.0 / 12.0 * (second - 2.0 * third + fourth) ** 2 + 0.25 * (second - fourth) ** 2
    smooth_c = 13.0 / 12.0 * (third - 2.0 * fourth + fifth) ** 2 + 0.25 * (3.0 * third - 4.0 * fourth + fifth) ** 2
    weight_a = 0.1 / (EPS_WENO + smooth_a) ** 2
    weight_b = 0.6 / (EPS_WENO + smooth_b) ** 2
    weight_c = 0.3 / (EPS_WENO + smooth_c) ** 2
    return (weight_a * cand_a + weight_b * cand_b + weight_c * cand_c) / (weight_a + weight_b + weight_c)

def divergence(padded, prims, alpha, var, axis_pos, count, cell_flag):
    flux = physical_flux(padded, prims, var)
    plus = 0.5 * (flux + alpha * padded)
    minus = 0.5 * (flux - alpha * padded)

    def window(arr, offset):
        return lax.slice_in_dim(arr, offset, offset + count + 1, axis=axis_pos)
    central = (37.0 * (window(flux, 2) + window(flux, 3)) - 8.0 * (window(flux, 1) + window(flux, 4)) + (window(flux, 0) + window(flux, 5))) / 60.0
    upwind = weno_face([window(plus, 0), window(plus, 1), window(plus, 2), window(plus, 3), window(plus, 4)])
    upwind = upwind + weno_face([window(minus, 5), window(minus, 4), window(minus, 3), window(minus, 2), window(minus, 1)])

    def jump(face):
        return lax.slice_in_dim(face, 1, count + 1, axis=axis_pos) - lax.slice_in_dim(face, 0, count, axis=axis_pos)
    return jnp.where(cell_flag[None], jump(upwind), jump(central))

def wall_pad(inner, top_ghost):
    mirror = jnp.array([1.0, 1.0, -1.0, 1.0, 1.0], dtype=jnp.float32).reshape(5, 1, 1, 1)
    lower = jnp.flip(inner[:, :, :3], axis=2) * mirror
    return jnp.concatenate([lower, inner, top_ghost], axis=2)

def expand_flags(flags):
    shape = flags.shape
    wide = jnp.broadcast_to(flags[:, :, :, None], (shape[0], shape[1], shape[2], ZBLOCK))
    return wide.reshape(shape[0], shape[1], shape[2] * ZBLOCK) > 0

def advance(inner, x_pad, z_pad, y_pad, register, cell_flag, alpha, x_prims):
    div_x = divergence(x_pad, x_prims, alpha[0], 1, 1, inner.shape[1], cell_flag)
    div_y = divergence(y_pad, primitives(y_pad), alpha[1], 2, 2, inner.shape[2], cell_flag)
    div_z = divergence(z_pad, primitives(z_pad), alpha[2], 3, 3, inner.shape[3], cell_flag)
    change = -(LAMBDA_X * div_x + LAMBDA_Y * div_y + LAMBDA_Z * div_z)
    new_register = REGISTER_DECAY * register + change
    new_state = inner + UPDATE_WEIGHT * new_register
    return (new_state, new_register)

def reference(state, register, top_ghost, flags):
    blocks = jnp.arange(N_GX, dtype=jnp.int32)

    def block_speeds(index):
        inner = lax.dynamic_slice_in_dim(state, index * CX, CX, 1)
        return local_speeds(primitives(inner))
    alpha = lax.optimization_barrier(jnp.max(lax.map(block_speeds, blocks), axis=0))

    def block_update(index):
        start = index * CX
        rows = (start - 3 + jnp.arange(CX + 6, dtype=jnp.int32)) % NX
        x_pad = jnp.take(state, rows.astype(jnp.int32), axis=1)
        inner = lax.dynamic_slice_in_dim(state, start, CX, 1)
        reg_block = lax.dynamic_slice_in_dim(register, start, CX, 1)
        top_block = lax.dynamic_slice_in_dim(top_ghost, start, CX, 1)
        flag_block = lax.dynamic_slice_in_dim(flags, start, CX, 0)
        z_pad = jnp.concatenate([inner[:, :, :, NZ - 3:], inner, inner[:, :, :, :3]], axis=3)
        y_pad = wall_pad(inner, top_block)
        return advance(inner, x_pad, z_pad, y_pad, reg_block, expand_flags(flag_block), alpha, primitives(x_pad))
    states, registers = lax.map(block_update, blocks)
    new_state = jnp.moveaxis(states, 0, 1).reshape(5, NX, NY, NZ)
    new_register = jnp.moveaxis(registers, 0, 1).reshape(5, NX, NY, NZ)
    return (new_state, new_register)
```

```python
import functools

import jax
import jax.numpy as jnp
from jax import lax
from jax.experimental import pallas as pl
from jax.experimental.pallas import tpu as pltpu
from jax.sharding import PartitionSpec as P

MESH = pl.DeviceIdType.MESH
GAMMA = 1.4
EPS_WENO = 1e-06
LAMBDA = (0.1, 0.15, 0.1)
REGISTER_DECAY = -5.0 / 9.0
UPDATE_WEIGHT = 15.0 / 16.0
UNROLL_LIMIT = 64


def reciprocal(value):
    return pltpu.reciprocal(value, approx=False)


def pressure_velocity(cons):
    inverse = reciprocal(cons[0])
    vel = [cons[1] * inverse, cons[2] * inverse, cons[3] * inverse]
    pressure = (GAMMA - 1.0) * (
        cons[4] - 0.5 * (cons[1] * vel[0] + cons[2] * vel[1] + cons[3] * vel[2])
    )
    return inverse, vel, pressure


def shifted(me, step, count):
    moved = me + step
    return jnp.where(moved >= count, moved - count, moved)


def exchange_peers(gx, gz, ngx, ngz):
    offsets = [(dx, dz) for dx in range(ngx) for dz in range(ngz)][1:]

    def each_peer(action):
        if len(offsets) < UNROLL_LIMIT:
            for slot, (dx, dz) in enumerate(offsets):
                action(slot, shifted(gx, dx, ngx), shifted(gz, dz, ngz))
        else:
            def body(slot, carry):
                dx, dz = (slot + 1) // ngz, (slot + 1) % ngz
                action(slot, shifted(gx, dx, ngx), shifted(gz, dz, ngz))
                return carry
            lax.fori_loop(0, len(offsets), body, 0)

    return each_peer, len(offsets)


class Line:
    def __init__(self, load):
        cached = functools.lru_cache(None)
        self.load = cached(load)
        self.D = cached(lambda j: self.load(j + 1) - self.load(j))
        self.S = cached(lambda j: self.D(j) - self.D(j - 1))
        self.T = cached(lambda j: self.S(j + 1) - self.S(j))
        self.S2 = cached(lambda j: self.S(j) + self.S(j))
        self.C = cached(
            lambda j: (self.S(j) * self.S(j) * (4.0 / 3.0) + 4.0 * EPS_WENO)
            + self.D(j) * self.D(j - 1)
        )

    def L(self, j):
        return self.C(j) + self.S2(j) * self.D(j)

    def R(self, j):
        return self.C(j) - self.S2(j) * self.D(j - 1)


def correction(near, mid, far, t_near, t_far):
    a, b, c = mid * far, near * far, near * mid
    w_near = a * a
    w_far = 3.0 * (c * c)
    total = w_near + 6.0 * (b * b) + w_far
    return (w_far * t_far + (w_near + w_near) * t_near) * reciprocal(total)


def upwind_gaps(alpha, load_flux, load_cons):
    flux = functools.lru_cache(None)(load_flux)
    drift = functools.lru_cache(None)(lambda j: alpha * load_cons(j))
    plus, minus = Line(lambda j: flux(j) + drift(j)), Line(lambda j: flux(j) - drift(j))

    def gap(j):
        up = correction(plus.L(j - 1), plus.C(j), plus.R(j + 1), plus.T(j - 1), plus.T(j))
        down = correction(minus.R(j + 2), minus.C(j + 1), minus.L(j), minus.T(j + 1), minus.T(j))
        return 0.5 * (plus.T(j) - minus.T(j)) - up + down

    return gap


def difference_weights(flagged):
    return (
        jnp.where(flagged, 8.0, 9.0),
        jnp.where(flagged, -1.0, -1.8),
        jnp.where(flagged, 0.0, 0.2),
    )


def linear_part(weights, flux, cell):
    total = None
    for reach, weight in enumerate(weights, 1):
        high, low = flux(cell + reach), flux(cell - reach)
        if high is None and low is None:
            continue
        gap = -low if high is None else high if low is None else high - low
        total = weight * gap if total is None else total + weight * gap
    return total


def fluxes_of(cons, var):
    _, vel, pressure = pressure_velocity(cons)
    velocity = vel[var - 1]
    fluxes = [cons[field] * velocity for field in range(4)]
    fluxes.append((cons[4] + pressure) * velocity)
    fluxes[var] = fluxes[var] + pressure
    return fluxes


def store_fluxes(cons, var, fluxes, conserved, cell):
    for field, flux in enumerate(fluxes_of(cons, var)):
        fluxes[field, cell] = flux
        conserved[field, cell] = cons[field]


def halo_fluxes(cx, ny, part, xpad, xf):
    for cell in (0, 1, 2, cx + 3, cx + 4, cx + 5):
        cons = [xpad[f, pl.ds(cell * ny + part * 8, 8), :] for f in range(5)]
        for field, flux in enumerate(fluxes_of(cons, 1)):
            xf[field, cell] = flux


def edge_update(cx, ny, part, f, alpha, xpad, xf, mask, acc, emit):
    rows = lambda cell: pl.ds(cell * ny + part * 8, 8)
    gap = upwind_gaps(alpha, lambda j: xf[f, j + 3], lambda j: xpad[f, rows(j + 3), :])
    outside = lambda j: xf[f, j + 3] if j < 0 or j >= cx else None
    for cell in range(cx):
        total = acc[f, rows(cell), :]
        if cell < 3 or cell >= cx - 3:
            scaled = mask[rows(cell), :]
            weights = difference_weights(scaled > 0.0)
            missing = linear_part([w * (LAMBDA[0] / 12.0) for w in weights], outside, cell)
            jump = None
            if cell < 2 or cell >= cx - 3:
                jump = gap(cell)
            if cell < 3 or cell > cx - 3:
                jump = -gap(cell - 1) if jump is None else jump - gap(cell - 1)
            total = total - (missing + scaled * jump)
        emit(cell, total)


def exchange_kernel(
    ngx, ngz, cx, ny, state_ref, register_ref, ghost_ref, flags_ref,
    acc, xpad, xf, mask, top_ref, early_register, early_state,
    zt, reg, ghost, flags, slots, mine, acc_t, zf, zu, yf, yu, xf_early,
    load_sem, side_sem, send_sem, recv_sem, halo_send, halo_recv
):
    gx, gz = lax.axis_index("gx"), lax.axis_index("gz")
    parts = ny // 8
    rows = cx * ny
    halo = 3 * ny
    strip = zt.shape[1] - 16
    chunk = strip // 8
    load = pltpu.make_async_copy(state_ref, xpad.at[:, pl.ds(halo, rows), :], load_sem)
    load.start()
    load_flags = pltpu.make_async_copy(flags_ref, flags, side_sem.at[0])
    load_flags.start()
    load_ghost = pltpu.make_async_copy(ghost_ref, ghost, side_sem.at[1])
    load_ghost.start()
    load_register = pltpu.make_async_copy(register_ref, reg, side_sem.at[2])
    load_register.start()
    barrier = pltpu.get_barrier_semaphore()
    each_peer, peers = exchange_peers(gx, gz, ngx, ngz)

    def greet(slot, tx, tz):
        pl.semaphore_signal(barrier, inc=1, device_id=(tx, tz), device_id_type=MESH)

    each_peer(greet)
    load.wait()
    best = None
    for row in range(0, rows, 8):
        cons = [xpad[var, pl.ds(halo + row, 8), :] for var in range(5)]
        inverse, vel, pressure = pressure_velocity(cons)
        sound = jnp.sqrt(GAMMA * pressure * inverse)
        local = [jnp.abs(v) + sound for v in vel]
        best = local if best is None else [jnp.maximum(a, b) for a, b in zip(best, local)]
    tops = [jnp.max(jnp.max(b, axis=0, keepdims=True), axis=1, keepdims=True) for b in best]
    lane = lax.broadcasted_iota(jnp.int32, (1, 128), 1)
    mine[...] = jnp.where(lane == 0, tops[0], jnp.where(lane == 1, tops[1], tops[2]))

    pl.semaphore_wait(barrier, peers)

    def send(slot, tx, tz):
        pltpu.make_async_remote_copy(
            src_ref=mine, dst_ref=slots.at[slot], send_sem=send_sem, recv_sem=recv_sem,
            device_id=(tx, tz), device_id_type=MESH,
        ).start()

    each_peer(send)
    right, left = shifted(gx, 1, ngx), shifted(gx, ngx - 1, ngx)
    high, low = shifted(gz, 1, ngz), shifted(gz, ngz - 1, ngz)

    def move(index, src, dst, target):
        copy = pltpu.make_async_remote_copy(
            src_ref=src, dst_ref=dst, send_sem=halo_send.at[index], recv_sem=halo_recv.at[index],
            device_id=target, device_id_type=MESH,
        )
        copy.start()
        return copy

    blocks = xpad.reshape(5, cx + 6, ny, xpad.shape[2])
    x_copies = []
    for part in range(parts):
        layers = lambda first: blocks.at[:, pl.ds(first, 3), pl.ds(part * 8, 8), :]
        x_copies.append((
            move(2 + 2 * part, layers(3), layers(3 + cx), (left, gz)),
            move(3 + 2 * part, layers(cx), layers(0), (right, gz)),
        ))
    for var in range(5):
        zt[var, pl.ds(8, strip), :] = xpad[var, pl.ds(halo, rows), :].T
    z_copies = [
        move(0, zt.at[:, pl.ds(8, 8), :], zt.at[:, pl.ds(8 + strip, 8), :], (gx, low)),
        move(1, zt.at[:, pl.ds(strip, 8), :], zt.at[:, pl.ds(0, 8), :], (gx, high)),
    ]
    load_flags.wait()
    for x in range(cx):
        wide = jnp.broadcast_to(flags[x], (strip, ny)).astype(jnp.float32).T * (LAMBDA[0] / 12.0)
        mask[pl.ds(x * ny, ny), :] = wide
    mask_t = mask[...].T[:8]
    flag_t = mask_t > 0.0

    load_ghost.wait()
    for cell in range(ny + 6):
        y = cell - 3
        if y < ny:
            source = y if y >= 0 else -1 - y
            cons = [xpad[f, pl.ds(halo + source, 8, stride=ny), :] for f in range(5)]
            if y < 0:
                cons[2] = -cons[2]
        else:
            cons = [ghost[f, y - ny] for f in range(5)]
        store_fluxes(cons, 2, yf, yu, cell)
    load_register.wait()

    def y_linear(f, carry):
        for cell in range(ny):
            where = pl.ds(cell, 8, stride=ny)
            weights = difference_weights(mask[where, :] > 0.0)
            linear = linear_part(weights, lambda j: yf[f, j + 3], cell)
            acc[f, where, :] = REGISTER_DECAY * reg[f, where, :] - (LAMBDA[1] / 12.0) * linear
        return carry

    lax.fori_loop(0, 5, y_linear, 0)
    for part in range(parts):
        target = xf if part == parts - 1 else xf_early.at[part]
        for cell in range(cx):
            cons = [xpad[f, pl.ds(halo + cell * ny + part * 8, 8), :] for f in range(5)]
            for field, flux in enumerate(fluxes_of(cons, 1)):
                target[field, 3 + cell] = flux

    def x_linear(f, carry):
        for part in range(parts):
            source = xf if part == parts - 1 else xf_early.at[part]
            inside = lambda j: source[f, j + 3] if 0 <= j < cx else None
            for cell in range(cx):
                where = pl.ds(cell * ny + part * 8, 8)
                weights = difference_weights(mask[where, :] > 0.0)
                linear = linear_part(weights, inside, cell)
                acc[f, where, :] = acc[f, where, :] - (LAMBDA[0] / 12.0) * linear
        return carry

    lax.fori_loop(0, 5, x_linear, 0)

    for copy in z_copies:
        copy.wait()
    for cell in range(chunk + 6):
        cons = [zt[f, pl.ds(5 + cell, 8, stride=chunk), :] for f in range(5)]
        store_fluxes(cons, 3, zf, zu, cell)
    weights_t = [w * (-LAMBDA[2] / 12.0) for w in difference_weights(flag_t)]

    def z_linear(f, carry):
        for cell in range(chunk):
            linear = linear_part(weights_t, lambda j: zf[f, j + 3], cell)
            acc_t[f, pl.ds(cell, 8, stride=chunk), :] = linear
        return carry

    lax.fori_loop(0, 5, z_linear, 0)

    pltpu.make_async_copy(slots, slots, recv_sem).wait()
    top = jnp.maximum(jnp.max(slots[...], axis=0), mine[...])
    top_ref[...] = jnp.broadcast_to(top, (8, 128))
    alpha = [jnp.broadcast_to(top[:, k : k + 1], (8, 128)) for k in range(3)]

    def z_field(f, carry):
        gap = upwind_gaps(alpha[2], lambda j: zf[f, j + 3], lambda j: zu[f, j + 3])
        before = gap(-1)
        for cell in range(chunk):
            after = gap(cell)
            where = pl.ds(cell, 8, stride=chunk)
            acc_t[f, where, :] = acc_t[f, where, :] - mask_t * (after - before)
            before = after
        return carry

    lax.fori_loop(0, 5, z_field, 0)

    def y_field(f, carry):
        gap = upwind_gaps(alpha[1], lambda j: yf[f, j + 3], lambda j: yu[f, j + 3])
        acc[f] = acc[f] + acc_t[f].T
        before = gap(-1)
        for cell in range(ny):
            after = gap(cell)
            where = pl.ds(cell, 8, stride=ny)
            scaled = (LAMBDA[1] / LAMBDA[0]) * mask[where, :]
            acc[f, where, :] = acc[f, where, :] - scaled * (after - before)
            before = after
        return carry

    lax.fori_loop(0, 5, y_field, 0)

    def x_field(f, carry):
        for part in range(parts):
            source = xf if part == parts - 1 else xf_early.at[part]
            at = lambda cell: pl.ds(cell * ny + part * 8, 8)
            gap = upwind_gaps(
                alpha[0], lambda j: source[f, j + 3], lambda j: xpad[f, at(j + 3), :]
            )
            for cell in range(2, cx - 2):
                if cell == 2:
                    jump = gap(2)
                elif cell == cx - 3:
                    jump = -gap(cell - 1)
                else:
                    jump = gap(cell) - gap(cell - 1)
                acc[f, at(cell), :] = acc[f, at(cell), :] - mask[at(cell), :] * jump
        return carry

    lax.fori_loop(0, 5, x_field, 0)

    for part in range(parts):
        for copy in x_copies[part]:
            copy.wait()
        if part < parts - 1:
            halo_fluxes(cx, ny, part, xpad, xf_early.at[part])

            def early(f, carry):
                def emit(cell, total):
                    state = xpad[f, pl.ds(halo + cell * ny + part * 8, 8), :]
                    early_register[part, f, cell] = total
                    early_state[part, f, cell] = state + UPDATE_WEIGHT * total
                edge_update(cx, ny, part, f, alpha[0], xpad, xf_early.at[part], mask, acc, emit)
                return carry

            lax.fori_loop(0, 5, early, 0)
    pltpu.make_async_copy(slots, slots, send_sem).wait()


def update_kernel(
    cx, ny, acc, xpad, xf_in, mask, top_ref, early_register, early_state,
    state_out, register_out, xf, late_register, late_state, sems
):
    parts = ny // 8
    part = parts - 1
    copies = []

    def put(src, dst):
        copy = pltpu.make_async_copy(src, dst, sems.at[len(copies)])
        copy.start()
        copies.append(copy)

    for p in range(parts - 1):
        put(early_register.at[p], register_out.at[:, :, pl.ds(p * 8, 8), :])
        put(early_state.at[p], state_out.at[:, :, pl.ds(p * 8, 8), :])
    halo_fluxes(cx, ny, part, xpad, xf)
    for f in range(5):
        for cell in range(3, cx + 3):
            xf[f, cell] = xf_in[f, cell]
    alpha = jnp.broadcast_to(top_ref[:, 0:1], (8, 128))
    for f in range(5):
        def emit(cell, total):
            state = xpad[f, pl.ds((3 + cell) * ny + part * 8, 8), :]
            late_register[f, cell] = total
            late_state[f, cell] = state + UPDATE_WEIGHT * total
        edge_update(cx, ny, part, f, alpha, xpad, xf, mask, acc, emit)
        put(late_register.at[f], register_out.at[f, :, pl.ds(part * 8, 8), :])
        put(late_state.at[f], state_out.at[f, :, pl.ds(part * 8, 8), :])
    for copy in copies:
        copy.wait()


def shards(ngx, ngz, state, register, top_ghost, flags):
    _, cx, ny, cz = state.shape
    rows = cx * ny
    parts = ny // 8
    peers = ngx * ngz - 1
    f32 = jnp.float32
    flat = lambda array: array.reshape(5, rows, cz)
    anywhere = pl.BlockSpec(memory_space=pl.ANY)
    inside = pl.BlockSpec(memory_space=pltpu.VMEM)
    held = pl.pallas_call(
        functools.partial(exchange_kernel, ngx, ngz, cx, ny),
        out_shape=(
            pltpu.VMEM((5, rows, cz), f32),
            pltpu.VMEM((5, (cx + 6) * ny, cz), f32),
            pltpu.VMEM((5, cx + 6, 8, cz), f32),
            pltpu.VMEM((rows, cz), f32),
            pltpu.VMEM((8, 128), f32),
            pltpu.VMEM((max(parts - 1, 1), 5, cx, 8, cz), f32),
            pltpu.VMEM((max(parts - 1, 1), 5, cx, 8, cz), f32),
        ),
        in_specs=[anywhere] * 4,
        out_specs=(inside,) * 7,
        scratch_shapes=[
            pltpu.VMEM((5, cz + 16, rows), f32),
            pltpu.VMEM((5, rows, cz), f32),
            pltpu.VMEM((5, 3, cx, cz), f32),
            pltpu.VMEM((cx, 1, ny), jnp.int32),
            pltpu.VMEM((peers, 1, 128), f32),
            pltpu.VMEM((1, 128), f32),
            pltpu.VMEM((5, cz, rows), f32),
            pltpu.VMEM((5, cz // 8 + 6, 8, rows), f32),
            pltpu.VMEM((5, cz // 8 + 6, 8, rows), f32),
            pltpu.VMEM((5, ny + 6, cx, cz), f32),
            pltpu.VMEM((5, ny + 6, cx, cz), f32),
            pltpu.VMEM((max(parts - 1, 1), 5, cx + 6, 8, cz), f32),
            pltpu.SemaphoreType.DMA,
            pltpu.SemaphoreType.DMA((3,)),
            pltpu.SemaphoreType.DMA,
            pltpu.SemaphoreType.DMA,
            pltpu.SemaphoreType.DMA((2 + 2 * parts,)),
            pltpu.SemaphoreType.DMA((2 + 2 * parts,)),
        ],
        compiler_params=pltpu.CompilerParams(collective_id=0, has_side_effects=True),
        name="exchange",
    )(flat(state), flat(register), top_ghost.transpose(0, 2, 1, 3), flags.transpose(0, 2, 1))
    block = jax.ShapeDtypeStruct(state.shape, f32)
    return pl.pallas_call(
        functools.partial(update_kernel, cx, ny),
        out_shape=(block, block),
        in_specs=[inside] * 7,
        out_specs=(anywhere, anywhere),
        scratch_shapes=[
            pltpu.VMEM((5, cx + 6, 8, cz), f32),
            pltpu.VMEM((5, cx, 8, cz), f32),
            pltpu.VMEM((5, cx, 8, cz), f32),
            pltpu.SemaphoreType.DMA((2 * (parts - 1) + 10,)),
        ],
        name="update",
    )(*(pltpu.with_memory_space_constraint(array, pltpu.VMEM) for array in held))


def solution(mesh):
    block = P(None, "gx", None, "gz")
    return jax.shard_map(
        functools.partial(shards, mesh.shape["gx"], mesh.shape["gz"]),
        mesh=mesh,
        in_specs=(block, block, block, P("gx", None, "gz")),
        out_specs=(block, block),
        check_vma=False,
    )
```

```python
import functools

import jax
import jax.numpy as jnp
from jax import lax
from jax.experimental import pallas as pl
from jax.experimental.pallas import tpu as pltpu
from jax.sharding import PartitionSpec as P

MESH = pl.DeviceIdType.MESH
GAMMA = 1.4
EPS_WENO = 1e-06
LAMBDA = (0.1, 0.15, 0.1)
REGISTER_DECAY = -5.0 / 9.0
UPDATE_WEIGHT = 15.0 / 16.0
UNROLL_LIMIT = 64
MID = 6.0**-0.5


def reciprocal(value):
    return pltpu.reciprocal(value, approx=False)


def pressure_velocity(cons):
    inverse = reciprocal(cons[0])
    vel = [cons[1] * inverse, cons[2] * inverse, cons[3] * inverse]
    pressure = (GAMMA - 1.0) * (
        cons[4] - 0.5 * (cons[1] * vel[0] + cons[2] * vel[1] + cons[3] * vel[2])
    )
    return inverse, vel, pressure


def shifted(me, step, count):
    moved = me + step
    return jnp.where(moved >= count, moved - count, moved)


def each(count, action, unroll):
    if unroll:
        for index in range(count):
            action(index)
    else:
        def body(index, carry):
            action(index)
            return carry
        lax.fori_loop(0, count, body, 0)


def plane_size(ngx):
    return max(p for p in range(1, ngx + 1) if ngx % p == 0 and p * p <= ngx)


class Peers:
    def __init__(self, ngx, ngz):
        self.ngx, self.ngz = ngx, ngz
        self.gx, self.gz = lax.axis_index("gx"), lax.axis_index("gz")
        self.wide = plane_size(ngx)
        self.planes = ngx // self.wide
        self.members = self.wide * ngz
        self.q, self.r = lax.div(self.gx, self.wide), lax.rem(self.gx, self.wide)
        self.own = self.r * ngz + self.gz
        self.last = self.gx == ngx - 1
        self.unroll = self.planes * self.members < UNROLL_LIMIT

    def member(self, plane, index):
        if isinstance(index, int):
            return plane * self.wide + index // self.ngz, index % self.ngz
        return plane * self.wide + lax.div(index, self.ngz), lax.rem(index, self.ngz)

    def plane_mates(self, action):
        def visit(index):
            @pl.when(self.own != index)
            def _():
                action(index, *self.member(self.q, index))
        each(self.members, visit, self.unroll)

    def of_planes(self, wanted, action):
        def visit(plane):
            @pl.when(wanted(plane))
            def _():
                each(self.members, lambda index: action(index, *self.member(plane, index)), self.unroll)
        each(self.planes, visit, self.unroll)

    def columns(self, wanted, action):
        def visit(plane):
            @pl.when(wanted(plane))
            def _():
                action(plane, (plane * self.wide + self.r, self.gz))
        each(self.planes, visit, self.unroll)

    def greet(self, barrier):
        def signal(tx, tz):
            pl.semaphore_signal(barrier, inc=1, device_id=(tx, tz), device_id_type=MESH)

        @pl.when((self.r == 0) & (self.gx > 0))
        def _():
            signal(self.gx - 1, self.gz)

        self.plane_mates(lambda index, tx, tz: signal(tx, tz))
        self.of_planes(lambda plane: plane > self.q, lambda index, tx, tz: signal(tx, tz))

    def greetings(self):
        has_next = (self.r == self.wide - 1) & jnp.logical_not(self.last)
        return self.members - 1 + self.q * self.members + has_next.astype(jnp.int32)


def cached(function):
    return functools.lru_cache(None)(function)


class Line:
    def __init__(self, load):
        self.load = cached(load)
        self.D = cached(lambda j: self.load(j + 1) - self.load(j))
        self.S = cached(lambda j: self.D(j) - self.D(j - 1))
        self.T = cached(lambda j: self.S(j + 1) - self.S(j))
        self.S2 = cached(lambda j: self.S(j) + self.S(j))
        self.C = cached(
            lambda j: (self.S(j) * self.S(j) * (4.0 / 3.0) + 4.0 * EPS_WENO)
            + self.D(j) * self.D(j - 1)
        )
        self.L = cached(lambda j: self.C(j) + self.S2(j) * self.D(j))
        self.M = cached(lambda j: MID * self.C(j))
        self.R = cached(lambda j: self.C(j) - self.S2(j) * self.D(j - 1))


def correction(near, mid, far, t_near, t_far):
    a, b, c = mid * far, near * far, near * mid
    w_near = a * a
    w_far = 3.0 * (c * c)
    total = w_near + b * b + w_far
    return (w_far * t_far + (w_near + w_near) * t_near) * reciprocal(total)


def face_gap(plus, minus, drift_t):
    def gap(j):
        up = correction(plus.L(j - 1), plus.M(j), plus.R(j + 1), plus.T(j - 1), plus.T(j))
        down = correction(minus.R(j + 2), minus.M(j + 1), minus.L(j), minus.T(j + 1), minus.T(j))
        return drift_t(j) - up + down

    return gap


KINDS = ("L", "M", "R")


def prepare(flux, cons, cells, store):
    f, u = Line(flux), Line(cons)
    for j in cells:
        mixed = (8.0 / 3.0) * (f.S(j) * u.S(j)) + (f.D(j) * u.D(j - 1) + f.D(j - 1) * u.D(j))
        curved = (4.0 / 3.0) * (u.S(j) * u.S(j)) + u.D(j) * u.D(j - 1)
        centre = (f.C(j), mixed, curved)

        def product(at):
            return (
                f.S2(j) * f.D(at),
                f.S2(j) * u.D(at) + u.S2(j) * f.D(at),
                u.S2(j) * u.D(at),
            )

        left = [c + p for c, p in zip(centre, product(j))]
        right = [c - p for c, p in zip(centre, product(j - 1))]
        for kind, terms in enumerate((left, [MID * c for c in centre], right)):
            for power, term in enumerate(terms):
                store(3 * kind + power, j, term)


def prepare_third(flux, cons, cells, store):
    f, u = Line(flux), Line(cons)
    for j in cells:
        store(9, j, f.T(j))
        store(10, j, u.T(j))


class Prepared:
    def __init__(self, alpha, load):
        square = alpha * alpha

        def both(kind):
            def pair(j):
                even = load(3 * kind, j) + square * load(3 * kind + 2, j)
                odd = alpha * load(3 * kind + 1, j)
                return even + odd, even - odd
            return cached(pair)

        self.drift_t = cached(lambda j: alpha * load(10, j))
        third = cached(lambda j: (load(9, j) + self.drift_t(j), load(9, j) - self.drift_t(j)))
        pairs = {name: both(kind) for kind, name in enumerate(KINDS)} | {"T": third}
        self.side = [
            {name: (lambda j, pair=pair, k=k: pair(j)[k]) for name, pair in pairs.items()} for k in range(2)
        ]


class Side:
    def __init__(self, values):
        self.L, self.M, self.R, self.T = (values[name] for name in (*KINDS, "T"))


def prepared_gaps(alpha, load):
    ready = Prepared(alpha, load)
    return face_gap(Side(ready.side[0]), Side(ready.side[1]), ready.drift_t)


def edge_gaps(alpha, load_flux, load_cons, load, inner, inner_t):
    flux = cached(load_flux)
    drift = cached(lambda j: alpha * load_cons(j))
    ready = Prepared(alpha, load)
    fresh = Line(lambda j: flux(j) + drift(j)), Line(lambda j: flux(j) - drift(j))

    def mixed(k):
        def pick(name):
            known = inner_t if name == "T" else inner
            return lambda j: ready.side[k][name](j) if j in known else getattr(fresh[k], name)(j)
        return Side({name: pick(name) for name in (*KINDS, "T")})

    plus, minus = mixed(0), mixed(1)

    def drift_t(j):
        return ready.drift_t(j) if j in inner_t else 0.5 * (plus.T(j) - minus.T(j))

    return face_gap(plus, minus, drift_t)


def difference_weights(flagged):
    return (
        jnp.where(flagged, 8.0, 9.0),
        jnp.where(flagged, -1.0, -1.8),
        jnp.where(flagged, 0.0, 0.2),
    )


def linear_part(weights, flux, cell):
    total = None
    for reach, weight in enumerate(weights, 1):
        high, low = flux(cell + reach), flux(cell - reach)
        if high is None and low is None:
            continue
        gap = -low if high is None else high if low is None else high - low
        total = weight * gap if total is None else total + weight * gap
    return total


def fluxes_of(cons, var):
    _, vel, pressure = pressure_velocity(cons)
    velocity = vel[var - 1]
    fluxes = [cons[field] * velocity for field in range(4)]
    fluxes.append((cons[4] + pressure) * velocity)
    fluxes[var] = fluxes[var] + pressure
    return fluxes


def store_fluxes(cons, var, fluxes, conserved, cell):
    for field, flux in enumerate(fluxes_of(cons, var)):
        fluxes[field, cell] = flux
        conserved[field, cell] = cons[field]


def prepare_line(count, f, fluxes, conserved, out):
    def keep(kind, j, value):
        out[kind, f, j + 2] = value

    flux, cons = cached(lambda j: fluxes[f, j + 3]), cached(lambda j: conserved[f, j + 3])
    prepare(flux, cons, range(-2, count + 2), keep)
    prepare_third(flux, cons, range(-2, count + 1), keep)


def halo_fluxes(cx, ny, part, xpad, xf):
    for cell in (0, 1, 2, cx + 3, cx + 4, cx + 5):
        cons = [xpad[f, pl.ds(cell * ny + part * 8, 8), :] for f in range(5)]
        for field, flux in enumerate(fluxes_of(cons, 1)):
            xf[field, cell] = flux


def edge_update(cx, ny, part, f, alpha, xpad, xf, mask, acc, near, emit):
    rows = lambda cell: pl.ds(cell * ny + part * 8, 8)
    gap = edge_gaps(
        alpha, lambda j: xf[f, j + 3], lambda j: xpad[f, rows(j + 3), :],
        lambda k, j: near[k, f, j - 1], range(1, cx - 1), range(1, cx - 2),
    )
    outside = lambda j: xf[f, j + 3] if j < 0 or j >= cx else None
    for cell in range(cx):
        total = acc[f, rows(cell), :]
        if cell < 3 or cell >= cx - 3:
            scaled = mask[rows(cell), :]
            weights = difference_weights(scaled > 0.0)
            missing = linear_part([w * (LAMBDA[0] / 12.0) for w in weights], outside, cell)
            jump = None
            if cell < 2 or cell >= cx - 3:
                jump = gap(cell)
            if cell < 3 or cell > cx - 3:
                jump = -gap(cell - 1) if jump is None else jump - gap(cell - 1)
            total = total - (missing + scaled * jump)
        emit(cell, total)


def exchange_kernel(
    ngx, ngz, cx, ny, state_ref, register_ref, ghost_ref, flags_ref,
    acc, xpad, xf, mask, top_ref, near, early_register, early_state,
    zt, reg, ghost, flags, slots, mine, plane_top, acc_t, zf, zu, yf, yu, xf_early, near_early, yq, zq,
    load_sem, side_sem, send_sem, recv_sem, halo_send, halo_recv, ready_up, ready_wrap
):
    peers = Peers(ngx, ngz)
    gx, gz = peers.gx, peers.gz
    parts = ny // 8
    rows = cx * ny
    halo = 3 * ny
    strip = zt.shape[1] - 16
    chunk = strip // 8
    load = pltpu.make_async_copy(state_ref, xpad.at[:, pl.ds(halo, rows), :], load_sem)
    load.start()
    load_flags = pltpu.make_async_copy(flags_ref, flags, side_sem.at[0])
    load_flags.start()
    load_ghost = pltpu.make_async_copy(ghost_ref, ghost, side_sem.at[1])
    load_ghost.start()
    load_register = pltpu.make_async_copy(register_ref, reg, side_sem.at[2])
    load_register.start()
    slots[...] = jnp.zeros(slots.shape, slots.dtype)
    barrier = pltpu.get_barrier_semaphore()
    peers.greet(barrier)
    load.wait()
    best = None
    for row in range(0, rows, 8):
        cons = [xpad[var, pl.ds(halo + row, 8), :] for var in range(5)]
        inverse, vel, pressure = pressure_velocity(cons)
        sound = jnp.sqrt(GAMMA * pressure * inverse)
        local = [jnp.abs(v) + sound for v in vel]
        best = local if best is None else [jnp.maximum(a, b) for a, b in zip(best, local)]
    tops = [jnp.max(jnp.max(b, axis=0, keepdims=True), axis=1, keepdims=True) for b in best]
    lane = lax.broadcasted_iota(jnp.int32, (1, 128), 1)
    mine[...] = jnp.where(lane == 0, tops[0], jnp.where(lane == 1, tops[1], tops[2]))

    right, left = shifted(gx, 1, ngx), shifted(gx, ngx - 1, ngx)
    high, low = shifted(gz, 1, ngz), shifted(gz, ngz - 1, ngz)

    def move(index, src, dst, target):
        return pltpu.make_async_remote_copy(
            src_ref=src, dst_ref=dst, send_sem=halo_send.at[index], recv_sem=halo_recv.at[index],
            device_id=target, device_id_type=MESH,
        )

    blocks = xpad.reshape(5, cx + 6, ny, xpad.shape[2])
    to_left, to_right = [], []
    for part in range(parts):
        layers = lambda first: blocks.at[:, pl.ds(first, 3), pl.ds(part * 8, 8), :]
        to_left.append(move(2 + 2 * part, layers(3), layers(3 + cx), (left, gz)))
        to_right.append(move(3 + 2 * part, layers(cx), layers(0), (right, gz)))

    def start(copies):
        for copy in copies:
            copy.start()

    def signal(semaphore, target):
        pl.semaphore_signal(semaphore, inc=1, device_id=target, device_id_type=MESH)

    def tell(source, plane, index, target):
        pltpu.make_async_remote_copy(
            src_ref=source, dst_ref=slots.at[peers.q, index], send_sem=send_sem.at[plane],
            recv_sem=recv_sem.at[peers.q], device_id=target, device_id_type=MESH,
        ).start()

    pl.semaphore_wait(barrier, peers.greetings())

    def tell_lower(plane):
        @pl.when(plane < peers.q)
        def _():
            each(
                peers.members,
                lambda index: tell(mine, plane, peers.own, peers.member(plane, index)),
                peers.unroll,
            )

    each(peers.planes, tell_lower, peers.unroll)
    peers.plane_mates(lambda index, tx, tz: tell(mine, peers.q, peers.own, (tx, tz)))

    @pl.when(peers.last)
    def _():
        start(to_right)
        signal(ready_wrap, (0, gz))

    @pl.when(gx > 0)
    def _():
        start(to_left)

    @pl.when(jnp.logical_not(peers.last))
    def _():
        start(to_right)

    peers.columns(lambda plane: plane < peers.q, lambda plane, target: signal(ready_up.at[peers.q], target))
    for var in range(5):
        zt[var, pl.ds(8, strip), :] = xpad[var, pl.ds(halo, rows), :].T
    z_copies = [
        move(0, zt.at[:, pl.ds(8, 8), :], zt.at[:, pl.ds(8 + strip, 8), :], (gx, low)),
        move(1, zt.at[:, pl.ds(strip, 8), :], zt.at[:, pl.ds(0, 8), :], (gx, high)),
    ]
    start(z_copies)
    load_flags.wait()
    for x in range(cx):
        wide = jnp.broadcast_to(flags[x], (strip, ny)).astype(jnp.float32).T * (LAMBDA[0] / 12.0)
        mask[pl.ds(x * ny, ny), :] = wide
    mask_t = mask[...].T[:8]
    flag_t = mask_t > 0.0

    load_ghost.wait()
    for cell in range(ny + 6):
        y = cell - 3
        if y < ny:
            source = y if y >= 0 else -1 - y
            cons = [xpad[f, pl.ds(halo + source, 8, stride=ny), :] for f in range(5)]
            if y < 0:
                cons[2] = -cons[2]
        else:
            cons = [ghost[f, y - ny] for f in range(5)]
        store_fluxes(cons, 2, yf, yu, cell)
    load_register.wait()

    def y_linear(f, carry):
        for cell in range(ny):
            where = pl.ds(cell, 8, stride=ny)
            weights = difference_weights(mask[where, :] > 0.0)
            linear = linear_part(weights, lambda j: yf[f, j + 3], cell)
            acc[f, where, :] = REGISTER_DECAY * reg[f, where, :] - (LAMBDA[1] / 12.0) * linear
        prepare_line(ny, f, yf, yu, yq)
        return carry

    lax.fori_loop(0, 5, y_linear, 0)
    for part in range(parts):
        target = xf if part == parts - 1 else xf_early.at[part]
        for cell in range(cx):
            cons = [xpad[f, pl.ds(halo + cell * ny + part * 8, 8), :] for f in range(5)]
            for field, flux in enumerate(fluxes_of(cons, 1)):
                target[field, 3 + cell] = flux

    def x_linear(f, carry):
        for part in range(parts):
            source = xf if part == parts - 1 else xf_early.at[part]
            found = near if part == parts - 1 else near_early.at[part]
            inside = lambda j: source[f, j + 3] if 0 <= j < cx else None

            def keep(kind, j, value):
                found[kind, f, j - 1] = value

            at = lambda j: pl.ds((j + 3) * ny + part * 8, 8)
            prepare(inside, lambda j: xpad[f, at(j), :], range(1, cx - 1), keep)
            prepare_third(inside, lambda j: xpad[f, at(j), :], range(1, cx - 2), keep)
            for cell in range(cx):
                where = pl.ds(cell * ny + part * 8, 8)
                weights = difference_weights(mask[where, :] > 0.0)
                linear = linear_part(weights, inside, cell)
                acc[f, where, :] = acc[f, where, :] - (LAMBDA[0] / 12.0) * linear
        return carry

    lax.fori_loop(0, 5, x_linear, 0)

    for copy in z_copies:
        copy.wait()
    for cell in range(chunk + 6):
        cons = [zt[f, pl.ds(5 + cell, 8, stride=chunk), :] for f in range(5)]
        store_fluxes(cons, 3, zf, zu, cell)
    weights_t = [w * (-LAMBDA[2] / 12.0) for w in difference_weights(flag_t)]

    def z_linear(f, carry):
        for cell in range(chunk):
            linear = linear_part(weights_t, lambda j: zf[f, j + 3], cell)
            acc_t[f, pl.ds(cell, 8, stride=chunk), :] = linear
        prepare_line(chunk, f, zf, zu, zq)
        return carry

    lax.fori_loop(0, 5, z_linear, 0)

    def all_of(plane, count, semaphores):
        some = slots.at[plane, pl.ds(0, count)]
        pltpu.make_async_copy(some, some, semaphores.at[plane]).wait()

    all_of(peers.q, peers.members - 1, recv_sem)
    plane_top[...] = jnp.maximum(jnp.max(slots[peers.q], axis=0), mine[...])

    def tell_higher(plane, target):
        pl.semaphore_wait(ready_up.at[plane], 1)
        tell(plane_top, plane, 0, target)

    peers.columns(lambda plane: plane > peers.q, tell_higher)

    @pl.when(gx == 0)
    def _():
        pl.semaphore_wait(ready_wrap, 1)
        start(to_left)

    def arrivals(plane):
        @pl.when(plane > peers.q)
        def _():
            all_of(plane, peers.members, recv_sem)

        @pl.when(plane < peers.q)
        def _():
            all_of(plane, 1, recv_sem)

    each(peers.planes, arrivals, peers.unroll)
    top = jnp.maximum(jnp.max(jnp.max(slots[...], axis=0), axis=0), mine[...])
    top_ref[...] = jnp.broadcast_to(top, (8, 128))
    alpha = [jnp.broadcast_to(top[:, k : k + 1], (8, 128)) for k in range(3)]

    def z_field(f, carry):
        gap = prepared_gaps(alpha[2], lambda k, j: zq[k, f, j + 2])
        before = gap(-1)
        for cell in range(chunk):
            after = gap(cell)
            where = pl.ds(cell, 8, stride=chunk)
            acc_t[f, where, :] = acc_t[f, where, :] - mask_t * (after - before)
            before = after
        return carry

    lax.fori_loop(0, 5, z_field, 0)

    def y_field(f, carry):
        gap = prepared_gaps(alpha[1], lambda k, j: yq[k, f, j + 2])
        acc[f] = acc[f] + acc_t[f].T
        before = gap(-1)
        for cell in range(ny):
            after = gap(cell)
            where = pl.ds(cell, 8, stride=ny)
            scaled = (LAMBDA[1] / LAMBDA[0]) * mask[where, :]
            acc[f, where, :] = acc[f, where, :] - scaled * (after - before)
            before = after
        return carry

    lax.fori_loop(0, 5, y_field, 0)

    def x_field(f, carry):
        for part in range(parts):
            found = near if part == parts - 1 else near_early.at[part]
            at = lambda cell: pl.ds(cell * ny + part * 8, 8)
            gap = prepared_gaps(alpha[0], lambda k, j: found[k, f, j - 1])
            for cell in range(2, cx - 2):
                if cell == 2:
                    jump = gap(2)
                elif cell == cx - 3:
                    jump = -gap(cell - 1)
                else:
                    jump = gap(cell) - gap(cell - 1)
                acc[f, at(cell), :] = acc[f, at(cell), :] - mask[at(cell), :] * jump
        return carry

    lax.fori_loop(0, 5, x_field, 0)

    for part in range(parts):
        to_left[part].wait()
        to_right[part].wait()
        if part < parts - 1:
            halo_fluxes(cx, ny, part, xpad, xf_early.at[part])

            def early(f, carry):
                def emit(cell, total):
                    state = xpad[f, pl.ds(halo + cell * ny + part * 8, 8), :]
                    early_register[part, f, cell] = total
                    early_state[part, f, cell] = state + UPDATE_WEIGHT * total
                edge_update(
                    cx, ny, part, f, alpha[0], xpad, xf_early.at[part], mask, acc, near_early.at[part], emit
                )
                return carry

            lax.fori_loop(0, 5, early, 0)

    def departures(plane):
        @pl.when(plane > peers.q)
        def _():
            all_of(plane, 1, send_sem)

        @pl.when(plane < peers.q)
        def _():
            all_of(plane, peers.members, send_sem)

    each(peers.planes, departures, peers.unroll)
    all_of(peers.q, peers.members - 1, send_sem)


def update_kernel(
    cx, ny, acc, xpad, xf_in, mask, top_ref, near, early_register, early_state,
    state_out, register_out, xf, late_register, late_state, sems
):
    parts = ny // 8
    part = parts - 1
    copies = []

    def put(src, dst):
        copy = pltpu.make_async_copy(src, dst, sems.at[len(copies)])
        copy.start()
        copies.append(copy)

    for p in range(parts - 1):
        put(early_register.at[p], register_out.at[:, :, pl.ds(p * 8, 8), :])
        put(early_state.at[p], state_out.at[:, :, pl.ds(p * 8, 8), :])
    halo_fluxes(cx, ny, part, xpad, xf)
    for f in range(5):
        for cell in range(3, cx + 3):
            xf[f, cell] = xf_in[f, cell]
    alpha = jnp.broadcast_to(top_ref[:, 0:1], (8, 128))
    for f in range(5):
        def emit(cell, total):
            state = xpad[f, pl.ds((3 + cell) * ny + part * 8, 8), :]
            late_register[f, cell] = total
            late_state[f, cell] = state + UPDATE_WEIGHT * total
        edge_update(cx, ny, part, f, alpha, xpad, xf, mask, acc, near, emit)
        put(late_register.at[f], register_out.at[f, :, pl.ds(part * 8, 8), :])
        put(late_state.at[f], state_out.at[f, :, pl.ds(part * 8, 8), :])
    for copy in copies:
        copy.wait()


def shards(ngx, ngz, state, register, top_ghost, flags):
    _, cx, ny, cz = state.shape
    rows = cx * ny
    parts = ny // 8
    wide = plane_size(ngx)
    f32 = jnp.float32
    flat = lambda array: array.reshape(5, rows, cz)
    anywhere = pl.BlockSpec(memory_space=pl.ANY)
    inside = pl.BlockSpec(memory_space=pltpu.VMEM)
    held = pl.pallas_call(
        functools.partial(exchange_kernel, ngx, ngz, cx, ny),
        out_shape=(
            pltpu.VMEM((5, rows, cz), f32),
            pltpu.VMEM((5, (cx + 6) * ny, cz), f32),
            pltpu.VMEM((5, cx + 6, 8, cz), f32),
            pltpu.VMEM((rows, cz), f32),
            pltpu.VMEM((8, 128), f32),
            pltpu.VMEM((11, 5, cx - 2, 8, cz), f32),
            pltpu.VMEM((max(parts - 1, 1), 5, cx, 8, cz), f32),
            pltpu.VMEM((max(parts - 1, 1), 5, cx, 8, cz), f32),
        ),
        in_specs=[anywhere] * 4,
        out_specs=(inside,) * 8,
        scratch_shapes=[
            pltpu.VMEM((5, cz + 16, rows), f32),
            pltpu.VMEM((5, rows, cz), f32),
            pltpu.VMEM((5, 3, cx, cz), f32),
            pltpu.VMEM((cx, 1, ny), jnp.int32),
            pltpu.VMEM((ngx // wide, wide * ngz, 1, 128), f32),
            pltpu.VMEM((1, 128), f32),
            pltpu.VMEM((1, 128), f32),
            pltpu.VMEM((5, cz, rows), f32),
            pltpu.VMEM((5, cz // 8 + 6, 8, rows), f32),
            pltpu.VMEM((5, cz // 8 + 6, 8, rows), f32),
            pltpu.VMEM((5, ny + 6, cx, cz), f32),
            pltpu.VMEM((5, ny + 6, cx, cz), f32),
            pltpu.VMEM((max(parts - 1, 1), 5, cx + 6, 8, cz), f32),
            pltpu.VMEM((max(parts - 1, 1), 11, 5, cx - 2, 8, cz), f32),
            pltpu.VMEM((11, 5, ny + 4, cx, cz), f32),
            pltpu.VMEM((11, 5, cz // 8 + 4, 8, rows), f32),
            pltpu.SemaphoreType.DMA,
            pltpu.SemaphoreType.DMA((3,)),
            pltpu.SemaphoreType.DMA((ngx // wide,)),
            pltpu.SemaphoreType.DMA((ngx // wide,)),
            pltpu.SemaphoreType.DMA((2 + 2 * parts,)),
            pltpu.SemaphoreType.DMA((2 + 2 * parts,)),
            pltpu.SemaphoreType.REGULAR((ngx // wide,)),
            pltpu.SemaphoreType.REGULAR,
        ],
        compiler_params=pltpu.CompilerParams(collective_id=0, has_side_effects=True),
        name="exchange",
    )(flat(state), flat(register), top_ghost.transpose(0, 2, 1, 3), flags.transpose(0, 2, 1))
    block = jax.ShapeDtypeStruct(state.shape, f32)
    return pl.pallas_call(
        functools.partial(update_kernel, cx, ny),
        out_shape=(block, block),
        in_specs=[inside] * 8,
        out_specs=(anywhere, anywhere),
        scratch_shapes=[
            pltpu.VMEM((5, cx + 6, 8, cz), f32),
            pltpu.VMEM((5, cx, 8, cz), f32),
            pltpu.VMEM((5, cx, 8, cz), f32),
            pltpu.SemaphoreType.DMA((2 * (parts - 1) + 10,)),
        ],
        name="update",
    )(*(pltpu.with_memory_space_constraint(array, pltpu.VMEM) for array in held))


def solution(mesh):
    block = P(None, "gx", None, "gz")
    return jax.shard_map(
        functools.partial(shards, mesh.shape["gx"], mesh.shape["gz"]),
        mesh=mesh,
        in_specs=(block, block, block, P("gx", None, "gz")),
        out_specs=(block, block),
        check_vma=False,
    )
```

```python
import functools

import jax
import jax.numpy as jnp
from jax import lax
from jax.experimental import pallas as pl
from jax.experimental.pallas import tpu as pltpu
from jax.sharding import PartitionSpec as P

MESH = pl.DeviceIdType.MESH
GAMMA = 1.4
EPS_WENO = 1e-06
LAMBDA = (0.1, 0.15, 0.1)
REGISTER_DECAY = -5.0 / 9.0
UPDATE_WEIGHT = 15.0 / 16.0
UNROLL_LIMIT = 64
MID = 6.0**-0.5


def reciprocal(value):
    return pltpu.reciprocal(value, approx=False)


def pressure_velocity(cons):
    inverse = reciprocal(cons[0])
    vel = [cons[1] * inverse, cons[2] * inverse, cons[3] * inverse]
    pressure = (GAMMA - 1.0) * (
        cons[4] - 0.5 * (cons[1] * vel[0] + cons[2] * vel[1] + cons[3] * vel[2])
    )
    return inverse, vel, pressure


def shifted(me, step, count):
    moved = me + step
    return jnp.where(moved >= count, moved - count, moved)


def each(count, action, unroll):
    if unroll:
        for index in range(count):
            action(index)
    else:
        def body(index, carry):
            action(index)
            return carry
        lax.fori_loop(0, count, body, 0)


def plane_size(ngx):
    return max(p for p in range(1, ngx + 1) if ngx % p == 0 and p * p <= ngx)


class Peers:
    def __init__(self, ngx, ngz):
        self.ngx, self.ngz = ngx, ngz
        self.gx, self.gz = lax.axis_index("gx"), lax.axis_index("gz")
        self.wide = plane_size(ngx)
        self.planes = ngx // self.wide
        self.members = self.wide * ngz
        self.q, self.r = lax.div(self.gx, self.wide), lax.rem(self.gx, self.wide)
        self.own = self.r * ngz + self.gz
        self.last = self.gx == ngx - 1
        self.unroll = self.planes * self.members < UNROLL_LIMIT

    def member(self, plane, index):
        if isinstance(index, int):
            return plane * self.wide + index // self.ngz, index % self.ngz
        return plane * self.wide + lax.div(index, self.ngz), lax.rem(index, self.ngz)

    def plane_mates(self, action):
        def visit(index):
            @pl.when(self.own != index)
            def _():
                action(index, *self.member(self.q, index))
        each(self.members, visit, self.unroll)

    def of_planes(self, wanted, action):
        def visit(plane):
            @pl.when(wanted(plane))
            def _():
                each(self.members, lambda index: action(index, *self.member(plane, index)), self.unroll)
        each(self.planes, visit, self.unroll)

    def columns(self, wanted, action):
        def visit(plane):
            @pl.when(wanted(plane))
            def _():
                action(plane, (plane * self.wide + self.r, self.gz))
        each(self.planes, visit, self.unroll)

    def greet(self, barrier):
        def signal(tx, tz):
            pl.semaphore_signal(barrier, inc=1, device_id=(tx, tz), device_id_type=MESH)

        @pl.when((self.r == 0) & (self.gx > 0))
        def _():
            signal(self.gx - 1, self.gz)

        self.plane_mates(lambda index, tx, tz: signal(tx, tz))
        self.of_planes(lambda plane: plane > self.q, lambda index, tx, tz: signal(tx, tz))

    def greetings(self):
        has_next = (self.r == self.wide - 1) & jnp.logical_not(self.last)
        return self.members - 1 + self.q * self.members + has_next.astype(jnp.int32)


def cached(function):
    return functools.lru_cache(None)(function)


class Line:
    def __init__(self, load):
        self.load = cached(load)
        self.D = cached(lambda j: self.load(j + 1) - self.load(j))
        self.S = cached(lambda j: self.D(j) - self.D(j - 1))
        self.T = cached(lambda j: self.S(j + 1) - self.S(j))
        self.S2 = cached(lambda j: self.S(j) + self.S(j))
        self.C = cached(
            lambda j: (self.S(j) * self.S(j) * (4.0 / 3.0) + 4.0 * EPS_WENO)
            + self.D(j) * self.D(j - 1)
        )
        self.L = cached(lambda j: self.C(j) + self.S2(j) * self.D(j))
        self.M = cached(lambda j: MID * self.C(j))
        self.R = cached(lambda j: self.C(j) - self.S2(j) * self.D(j - 1))


def correction(near, mid, far, t_near, t_far):
    a, b, c = mid * far, near * far, near * mid
    w_near = a * a
    w_far = 3.0 * (c * c)
    total = w_near + b * b + w_far
    return (w_far * t_far + (w_near + w_near) * t_near) * reciprocal(total)


def face_gap(plus, minus, drift_t):
    def gap(j):
        up = correction(plus.L(j - 1), plus.M(j), plus.R(j + 1), plus.T(j - 1), plus.T(j))
        down = correction(minus.R(j + 2), minus.M(j + 1), minus.L(j), minus.T(j + 1), minus.T(j))
        return drift_t(j) - up + down

    return gap


KINDS = ("L", "M", "R")


def prepare(flux, cons, cells, store):
    f, u = Line(flux), Line(cons)
    for j in cells:
        mixed = (8.0 / 3.0) * (f.S(j) * u.S(j)) + (f.D(j) * u.D(j - 1) + f.D(j - 1) * u.D(j))
        curved = (4.0 / 3.0) * (u.S(j) * u.S(j)) + u.D(j) * u.D(j - 1)
        centre = (f.C(j), mixed, curved)

        def product(at):
            return (
                f.S2(j) * f.D(at),
                f.S2(j) * u.D(at) + u.S2(j) * f.D(at),
                u.S2(j) * u.D(at),
            )

        left = [c + p for c, p in zip(centre, product(j))]
        right = [c - p for c, p in zip(centre, product(j - 1))]
        for kind, terms in enumerate((left, [MID * c for c in centre], right)):
            for power, term in enumerate(terms):
                store(3 * kind + power, j, term)


def prepare_third(flux, cons, cells, store):
    f, u = Line(flux), Line(cons)
    for j in cells:
        store(9, j, f.T(j))
        store(10, j, u.T(j))


class Prepared:
    def __init__(self, alpha, load):
        square = alpha * alpha

        def both(kind):
            def pair(j):
                even = load(3 * kind, j) + square * load(3 * kind + 2, j)
                odd = alpha * load(3 * kind + 1, j)
                return even + odd, even - odd
            return cached(pair)

        self.drift_t = cached(lambda j: alpha * load(10, j))
        third = cached(lambda j: (load(9, j) + self.drift_t(j), load(9, j) - self.drift_t(j)))
        pairs = {name: both(kind) for kind, name in enumerate(KINDS)} | {"T": third}
        self.side = [
            {name: (lambda j, pair=pair, k=k: pair(j)[k]) for name, pair in pairs.items()} for k in range(2)
        ]


class Side:
    def __init__(self, values):
        self.L, self.M, self.R, self.T = (values[name] for name in (*KINDS, "T"))


def prepared_gaps(alpha, load):
    ready = Prepared(alpha, load)
    return face_gap(Side(ready.side[0]), Side(ready.side[1]), ready.drift_t)


def edge_gaps(alpha, load_flux, load_cons, load, inner, inner_t):
    flux = cached(load_flux)
    drift = cached(lambda j: alpha * load_cons(j))
    ready = Prepared(alpha, load)
    fresh = Line(lambda j: flux(j) + drift(j)), Line(lambda j: flux(j) - drift(j))

    def mixed(k):
        def pick(name):
            known = inner_t if name == "T" else inner
            return lambda j: ready.side[k][name](j) if j in known else getattr(fresh[k], name)(j)
        return Side({name: pick(name) for name in (*KINDS, "T")})

    plus, minus = mixed(0), mixed(1)

    def drift_t(j):
        return ready.drift_t(j) if j in inner_t else 0.5 * (plus.T(j) - minus.T(j))

    return face_gap(plus, minus, drift_t)


def difference_weights(flagged):
    return (
        jnp.where(flagged, 8.0, 9.0),
        jnp.where(flagged, -1.0, -1.8),
        jnp.where(flagged, 0.0, 0.2),
    )


def linear_part(weights, flux, cell):
    total = None
    for reach, weight in enumerate(weights, 1):
        high, low = flux(cell + reach), flux(cell - reach)
        if high is None and low is None:
            continue
        gap = -low if high is None else high if low is None else high - low
        total = weight * gap if total is None else total + weight * gap
    return total


def fluxes_of(cons, var):
    _, vel, pressure = pressure_velocity(cons)
    velocity = vel[var - 1]
    fluxes = [cons[field] * velocity for field in range(4)]
    fluxes.append((cons[4] + pressure) * velocity)
    fluxes[var] = fluxes[var] + pressure
    return fluxes


def store_fluxes(cons, var, fluxes, conserved, cell):
    for field, flux in enumerate(fluxes_of(cons, var)):
        fluxes[field, cell] = flux
        conserved[field, cell] = cons[field]


def prepare_line(count, f, fluxes, conserved, out):
    def keep(kind, j, value):
        out[kind, f, j + 2] = value

    flux, cons = cached(lambda j: fluxes[f, j + 3]), cached(lambda j: conserved[f, j + 3])
    prepare(flux, cons, range(-2, count + 2), keep)
    prepare_third(flux, cons, range(-2, count + 1), keep)


def halo_fluxes(cx, ny, part, xpad, xf):
    for cell in (0, 1, 2, cx + 3, cx + 4, cx + 5):
        cons = [xpad[f, pl.ds(cell * ny + part * 8, 8), :] for f in range(5)]
        for field, flux in enumerate(fluxes_of(cons, 1)):
            xf[field, cell] = flux


def edge_update(cx, ny, part, f, alpha, xpad, xf, mask, acc, near, emit):
    rows = lambda cell: pl.ds(cell * ny + part * 8, 8)
    gap = edge_gaps(
        alpha, lambda j: xf[f, j + 3], lambda j: xpad[f, rows(j + 3), :],
        lambda k, j: near[k, f, j - 1], range(1, cx - 1), range(1, cx - 2),
    )
    outside = lambda j: xf[f, j + 3] if j < 0 or j >= cx else None
    for cell in range(cx):
        total = acc[f, rows(cell), :]
        if cell < 3 or cell >= cx - 3:
            scaled = mask[rows(cell), :]
            weights = difference_weights(scaled > 0.0)
            missing = linear_part([w * (LAMBDA[0] / 12.0) for w in weights], outside, cell)
            jump = None
            if cell < 2 or cell >= cx - 3:
                jump = gap(cell)
            if cell < 3 or cell > cx - 3:
                jump = -gap(cell - 1) if jump is None else jump - gap(cell - 1)
            total = total - (missing + scaled * jump)
        emit(cell, total)


def exchange_kernel(
    ngx, ngz, cx, ny, state_ref, register_ref, ghost_ref, flags_ref,
    acc, xpad, xf, mask, top_ref, near, early_register, early_state,
    zt, reg, ghost, flags, slots, mine, plane_top, acc_t, zf, zu, yf, yu, xf_early, near_early, yq, zq, y_base, z_base, y_mask, y_sum,
    load_sem, side_sem, send_sem, recv_sem, halo_send, halo_recv, ready_up, ready_wrap
):
    peers = Peers(ngx, ngz)
    gx, gz = peers.gx, peers.gz
    parts = ny // 8
    rows = cx * ny
    halo = 3 * ny
    strip = zt.shape[1] - 16
    chunk = strip // 8
    load = pltpu.make_async_copy(state_ref, xpad.at[:, pl.ds(halo, rows), :], load_sem)
    load.start()
    load_flags = pltpu.make_async_copy(flags_ref, flags, side_sem.at[0])
    load_flags.start()
    load_ghost = pltpu.make_async_copy(ghost_ref, ghost, side_sem.at[1])
    load_ghost.start()
    load_register = pltpu.make_async_copy(register_ref, reg, side_sem.at[2])
    load_register.start()
    slots[...] = jnp.zeros(slots.shape, slots.dtype)
    barrier = pltpu.get_barrier_semaphore()
    peers.greet(barrier)
    load.wait()
    best = None
    for row in range(0, rows, 8):
        cons = [xpad[var, pl.ds(halo + row, 8), :] for var in range(5)]
        inverse, vel, pressure = pressure_velocity(cons)
        sound = jnp.sqrt(GAMMA * pressure * inverse)
        local = [jnp.abs(v) + sound for v in vel]
        best = local if best is None else [jnp.maximum(a, b) for a, b in zip(best, local)]
    tops = [jnp.max(jnp.max(b, axis=0, keepdims=True), axis=1, keepdims=True) for b in best]
    lane = lax.broadcasted_iota(jnp.int32, (1, 128), 1)
    mine[...] = jnp.where(lane == 0, tops[0], jnp.where(lane == 1, tops[1], tops[2]))

    right, left = shifted(gx, 1, ngx), shifted(gx, ngx - 1, ngx)
    high, low = shifted(gz, 1, ngz), shifted(gz, ngz - 1, ngz)

    def move(index, src, dst, target):
        return pltpu.make_async_remote_copy(
            src_ref=src, dst_ref=dst, send_sem=halo_send.at[index], recv_sem=halo_recv.at[index],
            device_id=target, device_id_type=MESH,
        )

    blocks = xpad.reshape(5, cx + 6, ny, xpad.shape[2])
    to_left, to_right = [], []
    for part in range(parts):
        layers = lambda first: blocks.at[:, pl.ds(first, 3), pl.ds(part * 8, 8), :]
        to_left.append(move(2 + 2 * part, layers(3), layers(3 + cx), (left, gz)))
        to_right.append(move(3 + 2 * part, layers(cx), layers(0), (right, gz)))

    def start(copies):
        for copy in copies:
            copy.start()

    def signal(semaphore, target):
        pl.semaphore_signal(semaphore, inc=1, device_id=target, device_id_type=MESH)

    def tell(source, plane, index, target):
        pltpu.make_async_remote_copy(
            src_ref=source, dst_ref=slots.at[peers.q, index], send_sem=send_sem.at[plane],
            recv_sem=recv_sem.at[peers.q], device_id=target, device_id_type=MESH,
        ).start()

    pl.semaphore_wait(barrier, peers.greetings())

    def tell_lower(plane):
        @pl.when(plane < peers.q)
        def _():
            each(
                peers.members,
                lambda index: tell(mine, plane, peers.own, peers.member(plane, index)),
                peers.unroll,
            )

    each(peers.planes, tell_lower, peers.unroll)
    peers.plane_mates(lambda index, tx, tz: tell(mine, peers.q, peers.own, (tx, tz)))

    @pl.when(peers.last)
    def _():
        start(to_right)
        signal(ready_wrap, (0, gz))

    @pl.when(gx > 0)
    def _():
        start(to_left)

    @pl.when(jnp.logical_not(peers.last))
    def _():
        start(to_right)

    peers.columns(lambda plane: plane < peers.q, lambda plane, target: signal(ready_up.at[peers.q], target))
    for var in range(5):
        zt[var, pl.ds(8, strip), :] = xpad[var, pl.ds(halo, rows), :].T
    z_copies = [
        move(0, zt.at[:, pl.ds(8, 8), :], zt.at[:, pl.ds(8 + strip, 8), :], (gx, low)),
        move(1, zt.at[:, pl.ds(strip, 8), :], zt.at[:, pl.ds(0, 8), :], (gx, high)),
    ]
    start(z_copies)
    load_flags.wait()
    for x in range(cx):
        wide = jnp.broadcast_to(flags[x], (strip, ny)).astype(jnp.float32).T * (LAMBDA[0] / 12.0)
        mask[pl.ds(x * ny, ny), :] = wide
    mask_t = mask[...].T[:8]
    flag_t = mask_t > 0.0

    load_ghost.wait()
    for cell in range(ny + 6):
        y = cell - 3
        if y < ny:
            source = y if y >= 0 else -1 - y
            cons = [xpad[f, pl.ds(halo + source, 8, stride=ny), :] for f in range(5)]
            if y < 0:
                cons[2] = -cons[2]
        else:
            cons = [ghost[f, y - ny] for f in range(5)]
        store_fluxes(cons, 2, yf, yu, cell)
    for cell in range(ny):
        y_mask[cell] = (LAMBDA[1] / LAMBDA[0]) * mask[pl.ds(cell, 8, stride=ny), :]

    def y_linear(f, carry):
        for cell in range(ny):
            weights = difference_weights(y_mask[cell] > 0.0)
            linear = linear_part(weights, lambda j: yf[f, j + 3], cell)
            y_base[f, cell] = (-LAMBDA[1] / 12.0) * linear
        prepare_line(ny, f, yf, yu, yq)
        return carry

    lax.fori_loop(0, 5, y_linear, 0)
    for part in range(parts):
        target = xf if part == parts - 1 else xf_early.at[part]
        for cell in range(cx):
            cons = [xpad[f, pl.ds(halo + cell * ny + part * 8, 8), :] for f in range(5)]
            for field, flux in enumerate(fluxes_of(cons, 1)):
                target[field, 3 + cell] = flux

    load_register.wait()

    def x_linear(f, carry):
        for part in range(parts):
            source = xf if part == parts - 1 else xf_early.at[part]
            found = near if part == parts - 1 else near_early.at[part]
            inside = lambda j: source[f, j + 3] if 0 <= j < cx else None

            def keep(kind, j, value):
                found[kind, f, j - 1] = value

            at = lambda j: pl.ds((j + 3) * ny + part * 8, 8)
            prepare(inside, lambda j: xpad[f, at(j), :], range(1, cx - 1), keep)
            prepare_third(inside, lambda j: xpad[f, at(j), :], range(1, cx - 2), keep)
            for cell in range(cx):
                where = pl.ds(cell * ny + part * 8, 8)
                weights = difference_weights(mask[where, :] > 0.0)
                linear = linear_part(weights, inside, cell)
                acc[f, where, :] = REGISTER_DECAY * reg[f, where, :] - (LAMBDA[0] / 12.0) * linear
        return carry

    lax.fori_loop(0, 5, x_linear, 0)

    for copy in z_copies:
        copy.wait()
    for cell in range(chunk + 6):
        cons = [zt[f, pl.ds(5 + cell, 8, stride=chunk), :] for f in range(5)]
        store_fluxes(cons, 3, zf, zu, cell)
    weights_t = [w * (-LAMBDA[2] / 12.0) for w in difference_weights(flag_t)]

    def z_linear(f, carry):
        for cell in range(chunk):
            linear = linear_part(weights_t, lambda j: zf[f, j + 3], cell)
            z_base[f, cell] = linear
        prepare_line(chunk, f, zf, zu, zq)
        return carry

    lax.fori_loop(0, 5, z_linear, 0)

    def all_of(plane, count, semaphores):
        some = slots.at[plane, pl.ds(0, count)]
        pltpu.make_async_copy(some, some, semaphores.at[plane]).wait()

    all_of(peers.q, peers.members - 1, recv_sem)
    plane_top[...] = jnp.maximum(jnp.max(slots[peers.q], axis=0), mine[...])

    def tell_higher(plane, target):
        pl.semaphore_wait(ready_up.at[plane], 1)
        tell(plane_top, plane, 0, target)

    peers.columns(lambda plane: plane > peers.q, tell_higher)

    @pl.when(gx == 0)
    def _():
        pl.semaphore_wait(ready_wrap, 1)
        start(to_left)

    def arrivals(plane):
        @pl.when(plane > peers.q)
        def _():
            all_of(plane, peers.members, recv_sem)

        @pl.when(plane < peers.q)
        def _():
            all_of(plane, 1, recv_sem)

    each(peers.planes, arrivals, peers.unroll)
    top = jnp.maximum(jnp.max(jnp.max(slots[...], axis=0), axis=0), mine[...])
    top_ref[...] = jnp.broadcast_to(top, (8, 128))
    alpha = [jnp.broadcast_to(top[:, k : k + 1], (8, 128)) for k in range(3)]

    def z_field(f, carry):
        gap = prepared_gaps(alpha[2], lambda k, j: zq[k, f, j + 2])
        before = gap(-1)
        for cell in range(chunk):
            after = gap(cell)
            where = pl.ds(cell, 8, stride=chunk)
            acc_t[f, where, :] = z_base[f, cell] - mask_t * (after - before)
            before = after
        return carry

    lax.fori_loop(0, 5, z_field, 0, unroll=True)

    def y_field(f, carry):
        gap = prepared_gaps(alpha[1], lambda k, j: yq[k, f, j + 2])
        acc[f] = acc[f] + acc_t[f].T
        before = gap(-1)
        for cell in range(ny):
            after = gap(cell)
            where = pl.ds(cell, 8, stride=ny)
            y_sum[f, where, :] = y_base[f, cell] - y_mask[cell] * (after - before)
            before = after
        return carry

    lax.fori_loop(0, 5, y_field, 0, unroll=True)

    def x_field(f, carry):
        for part in range(parts):
            found = near if part == parts - 1 else near_early.at[part]
            at = lambda cell: pl.ds(cell * ny + part * 8, 8)
            gap = prepared_gaps(alpha[0], lambda k, j: found[k, f, j - 1])
            for cell in range(cx):
                total = acc[f, at(cell), :] + y_sum[f, at(cell), :]
                jump = None
                if 2 <= cell < cx - 3:
                    jump = gap(cell)
                if 2 < cell <= cx - 3:
                    jump = -gap(cell - 1) if jump is None else jump - gap(cell - 1)
                acc[f, at(cell), :] = total if jump is None else total - mask[at(cell), :] * jump
        return carry

    lax.fori_loop(0, 5, x_field, 0, unroll=True)

    for part in range(parts):
        to_left[part].wait()
        to_right[part].wait()
        if part < parts - 1:
            halo_fluxes(cx, ny, part, xpad, xf_early.at[part])

            def early(f, carry):
                def emit(cell, total):
                    state = xpad[f, pl.ds(halo + cell * ny + part * 8, 8), :]
                    early_register[part, f, cell] = total
                    early_state[part, f, cell] = state + UPDATE_WEIGHT * total
                edge_update(
                    cx, ny, part, f, alpha[0], xpad, xf_early.at[part], mask, acc, near_early.at[part], emit
                )
                return carry

            lax.fori_loop(0, 5, early, 0, unroll=True)

    def departures(plane):
        @pl.when(plane > peers.q)
        def _():
            all_of(plane, 1, send_sem)

        @pl.when(plane < peers.q)
        def _():
            all_of(plane, peers.members, send_sem)

    each(peers.planes, departures, peers.unroll)
    all_of(peers.q, peers.members - 1, send_sem)


def update_kernel(
    cx, ny, acc, xpad, xf_in, mask, top_ref, near, early_register, early_state,
    state_out, register_out, xf, late_register, late_state, sems
):
    parts = ny // 8
    part = parts - 1
    copies = []

    def put(src, dst):
        copy = pltpu.make_async_copy(src, dst, sems.at[len(copies)])
        copy.start()
        copies.append(copy)

    for p in range(parts - 1):
        put(early_register.at[p], register_out.at[:, :, pl.ds(p * 8, 8), :])
        put(early_state.at[p], state_out.at[:, :, pl.ds(p * 8, 8), :])
    halo_fluxes(cx, ny, part, xpad, xf)
    for f in range(5):
        for cell in range(3, cx + 3):
            xf[f, cell] = xf_in[f, cell]
    alpha = jnp.broadcast_to(top_ref[:, 0:1], (8, 128))
    for f in range(5):
        def emit(cell, total):
            state = xpad[f, pl.ds((3 + cell) * ny + part * 8, 8), :]
            late_register[f, cell] = total
            late_state[f, cell] = state + UPDATE_WEIGHT * total
        edge_update(cx, ny, part, f, alpha, xpad, xf, mask, acc, near, emit)
        put(late_register.at[f], register_out.at[f, :, pl.ds(part * 8, 8), :])
        put(late_state.at[f], state_out.at[f, :, pl.ds(part * 8, 8), :])
    for copy in copies:
        copy.wait()


def shards(ngx, ngz, state, register, top_ghost, flags):
    _, cx, ny, cz = state.shape
    rows = cx * ny
    parts = ny // 8
    wide = plane_size(ngx)
    f32 = jnp.float32
    flat = lambda array: array.reshape(5, rows, cz)
    anywhere = pl.BlockSpec(memory_space=pl.ANY)
    inside = pl.BlockSpec(memory_space=pltpu.VMEM)
    held = pl.pallas_call(
        functools.partial(exchange_kernel, ngx, ngz, cx, ny),
        out_shape=(
            pltpu.VMEM((5, rows, cz), f32),
            pltpu.VMEM((5, (cx + 6) * ny, cz), f32),
            pltpu.VMEM((5, cx + 6, 8, cz), f32),
            pltpu.VMEM((rows, cz), f32),
            pltpu.VMEM((8, 128), f32),
            pltpu.VMEM((11, 5, cx - 2, 8, cz), f32),
            pltpu.VMEM((max(parts - 1, 1), 5, cx, 8, cz), f32),
            pltpu.VMEM((max(parts - 1, 1), 5, cx, 8, cz), f32),
        ),
        in_specs=[anywhere] * 4,
        out_specs=(inside,) * 8,
        scratch_shapes=[
            pltpu.VMEM((5, cz + 16, rows), f32),
            pltpu.VMEM((5, rows, cz), f32),
            pltpu.VMEM((5, 3, cx, cz), f32),
            pltpu.VMEM((cx, 1, ny), jnp.int32),
            pltpu.VMEM((ngx // wide, wide * ngz, 1, 128), f32),
            pltpu.VMEM((1, 128), f32),
            pltpu.VMEM((1, 128), f32),
            pltpu.VMEM((5, cz, rows), f32),
            pltpu.VMEM((5, cz // 8 + 6, 8, rows), f32),
            pltpu.VMEM((5, cz // 8 + 6, 8, rows), f32),
            pltpu.VMEM((5, ny + 6, cx, cz), f32),
            pltpu.VMEM((5, ny + 6, cx, cz), f32),
            pltpu.VMEM((max(parts - 1, 1), 5, cx + 6, 8, cz), f32),
            pltpu.VMEM((max(parts - 1, 1), 11, 5, cx - 2, 8, cz), f32),
            pltpu.VMEM((11, 5, ny + 4, cx, cz), f32),
            pltpu.VMEM((11, 5, cz // 8 + 4, 8, rows), f32),
            pltpu.VMEM((5, ny, cx, cz), f32),
            pltpu.VMEM((5, cz // 8, 8, rows), f32),
            pltpu.VMEM((ny, cx, cz), f32),
            pltpu.VMEM((5, rows, cz), f32),
            pltpu.SemaphoreType.DMA,
            pltpu.SemaphoreType.DMA((3,)),
            pltpu.SemaphoreType.DMA((ngx // wide,)),
            pltpu.SemaphoreType.DMA((ngx // wide,)),
            pltpu.SemaphoreType.DMA((2 + 2 * parts,)),
            pltpu.SemaphoreType.DMA((2 + 2 * parts,)),
            pltpu.SemaphoreType.REGULAR((ngx // wide,)),
            pltpu.SemaphoreType.REGULAR,
        ],
        compiler_params=pltpu.CompilerParams(collective_id=0, has_side_effects=True),
        name="exchange",
    )(flat(state), flat(register), top_ghost.transpose(0, 2, 1, 3), flags.transpose(0, 2, 1))
    block = jax.ShapeDtypeStruct(state.shape, f32)
    return pl.pallas_call(
        functools.partial(update_kernel, cx, ny),
        out_shape=(block, block),
        in_specs=[inside] * 8,
        out_specs=(anywhere, anywhere),
        scratch_shapes=[
            pltpu.VMEM((5, cx + 6, 8, cz), f32),
            pltpu.VMEM((5, cx, 8, cz), f32),
            pltpu.VMEM((5, cx, 8, cz), f32),
            pltpu.SemaphoreType.DMA((2 * (parts - 1) + 10,)),
        ],
        name="update",
    )(*(pltpu.with_memory_space_constraint(array, pltpu.VMEM) for array in held))


def solution(mesh):
    block = P(None, "gx", None, "gz")
    return jax.shard_map(
        functools.partial(shards, mesh.shape["gx"], mesh.shape["gz"]),
        mesh=mesh,
        in_specs=(block, block, block, P("gx", None, "gz")),
        out_specs=(block, block),
        check_vma=False,
    )
```

```python
import functools

import jax
import jax.numpy as jnp
from jax import lax
from jax.experimental import pallas as pl
from jax.experimental.pallas import tpu as pltpu
from jax.sharding import PartitionSpec as P

MESH = pl.DeviceIdType.MESH
GAMMA = 1.4
EPS_WENO = 1e-06
LAMBDA = (0.1, 0.15, 0.1)
REGISTER_DECAY = -5.0 / 9.0
UPDATE_WEIGHT = 15.0 / 16.0
UNROLL_LIMIT = 64
MID = 6.0**-0.5


def reciprocal(value):
    return pltpu.reciprocal(value, approx=False)


def pressure_velocity(cons):
    inverse = reciprocal(cons[0])
    vel = [cons[1] * inverse, cons[2] * inverse, cons[3] * inverse]
    pressure = (GAMMA - 1.0) * (
        cons[4] - 0.5 * (cons[1] * vel[0] + cons[2] * vel[1] + cons[3] * vel[2])
    )
    return inverse, vel, pressure


def shifted(me, step, count):
    moved = me + step
    return jnp.where(moved >= count, moved - count, moved)


def each(count, action, unroll):
    if unroll:
        for index in range(count):
            action(index)
    else:
        def body(index, carry):
            action(index)
            return carry
        lax.fori_loop(0, count, body, 0)


def plane_size(ngx):
    return max(p for p in range(1, ngx + 1) if ngx % p == 0 and p * p <= ngx)


class Peers:
    def __init__(self, ngx, ngz):
        self.ngx, self.ngz = ngx, ngz
        self.gx, self.gz = lax.axis_index("gx"), lax.axis_index("gz")
        self.wide = plane_size(ngx)
        self.planes = ngx // self.wide
        self.members = self.wide * ngz
        self.q, self.r = lax.div(self.gx, self.wide), lax.rem(self.gx, self.wide)
        self.own = self.r * ngz + self.gz
        self.last = self.gx == ngx - 1
        self.unroll = self.planes * self.members < UNROLL_LIMIT

    def member(self, plane, index):
        if isinstance(index, int):
            return plane * self.wide + index // self.ngz, index % self.ngz
        return plane * self.wide + lax.div(index, self.ngz), lax.rem(index, self.ngz)

    def plane_mates(self, action):
        def visit(index):
            @pl.when(self.own != index)
            def _():
                action(index, *self.member(self.q, index))
        each(self.members, visit, self.unroll)

    def of_planes(self, wanted, action):
        def visit(plane):
            @pl.when(wanted(plane))
            def _():
                each(self.members, lambda index: action(index, *self.member(plane, index)), self.unroll)
        each(self.planes, visit, self.unroll)

    def columns(self, wanted, action):
        def visit(plane):
            @pl.when(wanted(plane))
            def _():
                action(plane, (plane * self.wide + self.r, self.gz))
        each(self.planes, visit, self.unroll)

    def greet(self, barrier):
        def signal(tx, tz):
            pl.semaphore_signal(barrier, inc=1, device_id=(tx, tz), device_id_type=MESH)

        @pl.when((self.r == 0) & (self.gx > 0))
        def _():
            signal(self.gx - 1, self.gz)

        self.plane_mates(lambda index, tx, tz: signal(tx, tz))
        self.of_planes(lambda plane: plane > self.q, lambda index, tx, tz: signal(tx, tz))

    def greetings(self):
        has_next = (self.r == self.wide - 1) & jnp.logical_not(self.last)
        return self.members - 1 + self.q * self.members + has_next.astype(jnp.int32)


def cached(function):
    return functools.lru_cache(None)(function)


class Line:
    def __init__(self, load):
        self.load = cached(load)
        self.D = cached(lambda j: self.load(j + 1) - self.load(j))
        self.S = cached(lambda j: self.D(j) - self.D(j - 1))
        self.T = cached(lambda j: self.S(j + 1) - self.S(j))
        self.S2 = cached(lambda j: self.S(j) + self.S(j))
        self.C = cached(
            lambda j: (self.S(j) * self.S(j) * (4.0 / 3.0) + 4.0 * EPS_WENO)
            + self.D(j) * self.D(j - 1)
        )
        self.L = cached(lambda j: self.C(j) + self.S2(j) * self.D(j))
        self.M = cached(lambda j: MID * self.C(j))
        self.R = cached(lambda j: self.C(j) - self.S2(j) * self.D(j - 1))


def correction(near, mid, far, t_near, t_far):
    a, b, c = mid * far, near * far, near * mid
    w_near = a * a
    w_far = 3.0 * (c * c)
    total = w_near + b * b + w_far
    return (w_far * t_far + (w_near + w_near) * t_near) * reciprocal(total)


def face_gap(plus, minus, drift_t):
    def gap(j):
        up = correction(plus.L(j - 1), plus.M(j), plus.R(j + 1), plus.T(j - 1), plus.T(j))
        down = correction(minus.R(j + 2), minus.M(j + 1), minus.L(j), minus.T(j + 1), minus.T(j))
        return drift_t(j) - up + down

    return gap


KINDS = ("L", "M", "R")


def prepare(flux, cons, cells, store):
    f, u = Line(flux), Line(cons)
    for j in cells:
        mixed = (8.0 / 3.0) * (f.S(j) * u.S(j)) + (f.D(j) * u.D(j - 1) + f.D(j - 1) * u.D(j))
        curved = (4.0 / 3.0) * (u.S(j) * u.S(j)) + u.D(j) * u.D(j - 1)
        centre = (f.C(j), mixed, curved)

        def product(at):
            return (
                f.S2(j) * f.D(at),
                f.S2(j) * u.D(at) + u.S2(j) * f.D(at),
                u.S2(j) * u.D(at),
            )

        left = [c + p for c, p in zip(centre, product(j))]
        right = [c - p for c, p in zip(centre, product(j - 1))]
        for kind, terms in enumerate((left, [MID * c for c in centre], right)):
            for power, term in enumerate(terms):
                store(3 * kind + power, j, term)


def prepare_third(flux, cons, cells, store, scale=1.0):
    f, u = Line(flux), Line(cons)
    for j in cells:
        store(9, j, f.T(j) if scale == 1.0 else scale * f.T(j))
        store(10, j, u.T(j) if scale == 1.0 else scale * u.T(j))


class Prepared:
    def __init__(self, alpha, load):
        square = alpha * alpha

        def both(kind):
            def pair(j):
                even = load(3 * kind, j) + square * load(3 * kind + 2, j)
                odd = alpha * load(3 * kind + 1, j)
                return even + odd, even - odd
            return cached(pair)

        self.drift_t = cached(lambda j: alpha * load(10, j))
        third = cached(lambda j: (load(9, j) + self.drift_t(j), load(9, j) - self.drift_t(j)))
        pairs = {name: both(kind) for kind, name in enumerate(KINDS)} | {"T": third}
        self.side = [
            {name: (lambda j, pair=pair, k=k: pair(j)[k]) for name, pair in pairs.items()} for k in range(2)
        ]


class Side:
    def __init__(self, values):
        self.L, self.M, self.R, self.T = (values[name] for name in (*KINDS, "T"))


def prepared_gaps(alpha, load):
    ready = Prepared(alpha, load)
    return face_gap(Side(ready.side[0]), Side(ready.side[1]), ready.drift_t)


def edge_gaps(alpha, load_flux, load_cons, load, inner, inner_t):
    flux = cached(load_flux)
    drift = cached(lambda j: alpha * load_cons(j))
    ready = Prepared(alpha, load)
    fresh = Line(lambda j: flux(j) + drift(j)), Line(lambda j: flux(j) - drift(j))

    def mixed(k):
        def pick(name):
            known = inner_t if name == "T" else inner
            return lambda j: ready.side[k][name](j) if j in known else getattr(fresh[k], name)(j)
        return Side({name: pick(name) for name in (*KINDS, "T")})

    plus, minus = mixed(0), mixed(1)

    def drift_t(j):
        return ready.drift_t(j) if j in inner_t else 0.5 * (plus.T(j) - minus.T(j))

    return face_gap(plus, minus, drift_t)


def difference_weights(flagged):
    return (
        jnp.where(flagged, 8.0, 9.0),
        jnp.where(flagged, -1.0, -1.8),
        jnp.where(flagged, 0.0, 0.2),
    )


def linear_part(weights, flux, cell):
    total = None
    for reach, weight in enumerate(weights, 1):
        high, low = flux(cell + reach), flux(cell - reach)
        if high is None and low is None:
            continue
        gap = -low if high is None else high if low is None else high - low
        total = weight * gap if total is None else total + weight * gap
    return total


def fluxes_of(cons, var):
    _, vel, pressure = pressure_velocity(cons)
    velocity = vel[var - 1]
    fluxes = [cons[field] * velocity for field in range(4)]
    fluxes.append((cons[4] + pressure) * velocity)
    fluxes[var] = fluxes[var] + pressure
    return fluxes


def store_fluxes(cons, var, fluxes, conserved, cell):
    for field, flux in enumerate(fluxes_of(cons, var)):
        fluxes[field, cell] = flux
        conserved[field, cell] = cons[field]


def prepare_line(count, scale, f, fluxes, conserved, out):
    def keep(kind, j, value):
        out[kind, f, j + 2] = value

    flux, cons = cached(lambda j: fluxes[f, j + 3]), cached(lambda j: conserved[f, j + 3])
    prepare(flux, cons, range(-2, count + 2), keep)
    prepare_third(flux, cons, range(-2, count + 1), keep, scale)


def store_x_fluxes(ny, part, cells, xpad, xf):
    for cell in cells:
        cons = [xpad[f, pl.ds((cell + 3) * ny + part * 8, 8), :] for f in range(5)]
        for field, flux in enumerate(fluxes_of(cons, 1)):
            xf[part, field, cell + 3] = flux


def left_edge(ny, part, alpha, xpad, flux, mask, acc, known, jumps, emit):
    rows = lambda cell: pl.ds(cell * ny + part * 8, 8)
    scaled = [mask[rows(cell), :] for cell in range(3)]
    weights = [
        [weight * (LAMBDA[0] / 12.0) for weight in difference_weights(m > 0.0)] for m in scaled
    ]
    for f in range(5):
        gap = edge_gaps(
            alpha, lambda j: flux(f, j), lambda j: xpad[f, rows(j + 3), :],
            lambda k, j: known(k, f, j), range(1, 4), range(1, 4),
        )
        outside = lambda j: flux(f, j) if j < 0 else None
        for cell in range(3):
            jump = jumps[f, rows(cell), :] - gap(cell - 1)
            if cell < 2:
                jump = jump + gap(cell)
            missing = linear_part(weights[cell], outside, cell)
            emit(f, cell, acc[f, rows(cell), :] - (missing + scaled[cell] * jump))


def exchange_kernel(
    ngx, ngz, cx, ny, state_ref, register_ref, ghost_ref, flags_ref,
    acc, xpad, mask, top_ref, edge_flux, edge_near, jumps, done_register, done_state,
    zt, reg, ghost, flags, slots, mine, plane_top, acc_t, zf, zu, yf, yu, yq, zq, xf, near,
    load_sem, side_sem, send_sem, recv_sem, halo_send, halo_recv, ready_up, ready_wrap
):
    peers = Peers(ngx, ngz)
    gx, gz = peers.gx, peers.gz
    parts = ny // 8
    rows = cx * ny
    halo = 3 * ny
    strip = zt.shape[1] - 16
    chunk = strip // 8
    load = pltpu.make_async_copy(state_ref, xpad.at[:, pl.ds(halo, rows), :], load_sem)
    load.start()
    load_flags = pltpu.make_async_copy(flags_ref, flags, side_sem.at[0])
    load_ghost = pltpu.make_async_copy(ghost_ref, ghost, side_sem.at[1])
    load_register = pltpu.make_async_copy(register_ref, reg, side_sem.at[2])
    slots[...] = jnp.zeros(slots.shape, slots.dtype)
    barrier = pltpu.get_barrier_semaphore()
    peers.greet(barrier)
    load.wait()
    load_flags.start()
    load_ghost.start()
    load_register.start()
    best = None
    for row in range(0, rows, 8):
        cons = [xpad[var, pl.ds(halo + row, 8), :] for var in range(5)]
        inverse, vel, pressure = pressure_velocity(cons)
        sound = jnp.sqrt(GAMMA * pressure * inverse)
        local = [jnp.abs(v) + sound for v in vel]
        best = local if best is None else [jnp.maximum(a, b) for a, b in zip(best, local)]
    tops = [jnp.max(jnp.max(b, axis=0, keepdims=True), axis=1, keepdims=True) for b in best]
    lane = lax.broadcasted_iota(jnp.int32, (1, 128), 1)
    mine[...] = jnp.where(lane == 0, tops[0], jnp.where(lane == 1, tops[1], tops[2]))

    right, left = shifted(gx, 1, ngx), shifted(gx, ngx - 1, ngx)
    high, low = shifted(gz, 1, ngz), shifted(gz, ngz - 1, ngz)

    def move(index, src, dst, target):
        return pltpu.make_async_remote_copy(
            src_ref=src, dst_ref=dst, send_sem=halo_send.at[index], recv_sem=halo_recv.at[index],
            device_id=target, device_id_type=MESH,
        )

    blocks = xpad.reshape(5, cx + 6, ny, xpad.shape[2])
    to_left, to_right = [], []
    for part in range(parts):
        layers = lambda first: blocks.at[:, pl.ds(first, 3), pl.ds(part * 8, 8), :]
        to_left.append(move(2 + 2 * part, layers(3), layers(3 + cx), (left, gz)))
        to_right.append(move(3 + 2 * part, layers(cx), layers(0), (right, gz)))

    def start(copies):
        for copy in copies:
            copy.start()

    def signal(semaphore, target):
        pl.semaphore_signal(semaphore, inc=1, device_id=target, device_id_type=MESH)

    def tell(source, plane, index, target):
        pltpu.make_async_remote_copy(
            src_ref=source, dst_ref=slots.at[peers.q, index], send_sem=send_sem.at[plane],
            recv_sem=recv_sem.at[peers.q], device_id=target, device_id_type=MESH,
        ).start()

    pl.semaphore_wait(barrier, peers.greetings())

    def tell_lower(plane):
        @pl.when(plane < peers.q)
        def _():
            each(
                peers.members,
                lambda index: tell(mine, plane, peers.own, peers.member(plane, index)),
                peers.unroll,
            )

    each(peers.planes, tell_lower, peers.unroll)
    peers.plane_mates(lambda index, tx, tz: tell(mine, peers.q, peers.own, (tx, tz)))

    yields = peers.last & (gz > 0)

    @pl.when(peers.last)
    def _():
        signal(ready_wrap, (0, gz))
        start(to_right[:1])

    @pl.when(peers.last & (gz == 0))
    def _():
        start(to_right[1:])

    @pl.when((gx > 0) & jnp.logical_not(yields))
    def _():
        start(to_left)

    @pl.when(jnp.logical_not(peers.last))
    def _():
        start(to_right)

    peers.columns(lambda plane: plane < peers.q, lambda plane, target: signal(ready_up.at[peers.q], target))
    for var in range(5):
        zt[var, pl.ds(8, strip), :] = xpad[var, pl.ds(halo, rows), :].T
    z_copies = [
        move(0, zt.at[:, pl.ds(8, 8), :], zt.at[:, pl.ds(8 + strip, 8), :], (gx, low)),
        move(1, zt.at[:, pl.ds(strip, 8), :], zt.at[:, pl.ds(0, 8), :], (gx, high)),
    ]
    start(z_copies)
    load_flags.wait()
    for x in range(cx):
        wide = jnp.broadcast_to(flags[x], (strip, ny)).astype(jnp.float32).T * (LAMBDA[0] / 12.0)
        mask[pl.ds(x * ny, ny), :] = wide
    mask_t = mask[...].T[:8]
    flag_t = mask_t > 0.0

    load_ghost.wait()
    for cell in range(ny + 6):
        y = cell - 3
        if y < ny:
            source = y if y >= 0 else -1 - y
            cons = [xpad[f, pl.ds(halo + source, 8, stride=ny), :] for f in range(5)]
            if y < 0:
                cons[2] = -cons[2]
        else:
            cons = [ghost[f, y - ny] for f in range(5)]
        store_fluxes(cons, 2, yf, yu, cell)
    load_register.wait()

    def y_linear(f, carry):
        for cell in range(ny):
            where = pl.ds(cell, 8, stride=ny)
            weights = difference_weights(mask[where, :] > 0.0)
            linear = linear_part(weights, lambda j: yf[f, j + 3], cell)
            acc[f, where, :] = REGISTER_DECAY * reg[f, where, :] - (LAMBDA[1] / 12.0) * linear
        prepare_line(ny, LAMBDA[1] / LAMBDA[0], f, yf, yu, yq)
        return carry

    lax.fori_loop(0, 5, y_linear, 0)

    @pl.when(yields)
    def _():
        start(to_right[1:])
        start(to_left)

    for part in range(parts):
        store_x_fluxes(ny, part, range(cx), xpad, xf)

    def x_prepare(f, part, centres, thirds):
        def keep(kind, j, value):
            near[part, kind, f, j - 1] = value

        flux = cached(lambda j: xf[part, f, j + 3])
        cons = cached(lambda j: xpad[f, pl.ds((j + 3) * ny + part * 8, 8), :])
        prepare(flux, cons, centres, keep)
        prepare_third(flux, cons, thirds, keep)

    def x_linear(f, part, cells, known):
        for cell in cells:
            where = pl.ds(cell * ny + part * 8, 8)
            weights = difference_weights(mask[where, :] > 0.0)
            linear = linear_part(weights, lambda j: xf[part, f, j + 3] if known(j) else None, cell)
            acc[f, where, :] = acc[f, where, :] - (LAMBDA[0] / 12.0) * linear

    def x_inner(f, carry):
        for part in range(parts):
            x_prepare(f, part, range(1, cx - 1), range(1, cx - 2))
            if part == parts - 1:
                for cell in range(5):
                    edge_flux[f, cell] = xf[part, f, cell + 3]
                for kind in range(11):
                    for j in range(1, 4):
                        edge_near[kind, f, j - 1] = near[part, kind, f, j - 1]
            x_linear(f, part, range(cx), lambda j: 0 <= j < cx)
        return carry

    lax.fori_loop(0, 5, x_inner, 0)

    def right_edge():
        for part in range(parts):
            to_left[part].wait_recv()
            store_x_fluxes(ny, part, range(cx, cx + 3), xpad, xf)

        def field(f, carry):
            for part in range(parts):
                x_prepare(f, part, range(cx - 1, cx + 2), range(cx - 2, cx + 1))
                x_linear(f, part, range(cx - 3, cx), lambda j: j >= cx)
            return carry

        lax.fori_loop(0, 5, field, 0)

    for copy in z_copies:
        copy.wait()
    for cell in range(chunk + 6):
        cons = [zt[f, pl.ds(5 + cell, 8, stride=chunk), :] for f in range(5)]
        store_fluxes(cons, 3, zf, zu, cell)
    weights_t = [w * (-LAMBDA[2] / 12.0) for w in difference_weights(flag_t)]

    def z_linear(f, carry):
        for cell in range(chunk):
            linear = linear_part(weights_t, lambda j: zf[f, j + 3], cell)
            acc_t[f, pl.ds(cell, 8, stride=chunk), :] = linear
        acc[f] = acc[f] + acc_t[f].T
        prepare_line(chunk, LAMBDA[2] / LAMBDA[0], f, zf, zu, zq)
        return carry

    lax.fori_loop(0, 5, z_linear, 0)

    def all_of(plane, count, semaphores):
        some = slots.at[plane, pl.ds(0, count)]
        pltpu.make_async_copy(some, some, semaphores.at[plane]).wait()

    all_of(peers.q, peers.members - 1, recv_sem)
    plane_top[...] = jnp.maximum(jnp.max(slots[peers.q], axis=0), mine[...])

    def tell_higher(plane, target):
        pl.semaphore_wait(ready_up.at[plane], 1)
        tell(plane_top, plane, 0, target)

    peers.columns(lambda plane: plane > peers.q, tell_higher)

    @pl.when(gx == 0)
    def _():
        pl.semaphore_wait(ready_wrap, 1)
        start(to_left)

    @pl.when(jnp.logical_not(peers.last))
    def _():
        right_edge()

    def arrivals(plane):
        @pl.when(plane > peers.q)
        def _():
            all_of(plane, peers.members, recv_sem)

        @pl.when(plane < peers.q)
        def _():
            all_of(plane, 1, recv_sem)

    each(peers.planes, arrivals, peers.unroll)
    top = jnp.maximum(jnp.max(jnp.max(slots[...], axis=0), axis=0), mine[...])
    top_ref[...] = jnp.broadcast_to(top, (8, 128))
    alpha = [jnp.broadcast_to(top[:, k : k + 1], (8, 128)) for k in range(3)]

    def z_field(f, carry):
        gap = prepared_gaps(alpha[2], lambda k, j: zq[k, f, j + 2])
        before = gap(-1)
        for cell in range(chunk):
            after = gap(cell)
            acc_t[f, pl.ds(cell, 8, stride=chunk), :] = after - before
            before = after
        return carry

    lax.fori_loop(0, 5, z_field, 0, unroll=True)

    def y_field(f, carry):
        gap = prepared_gaps(alpha[1], lambda k, j: yq[k, f, j + 2])
        before = gap(-1)
        for cell in range(ny):
            after = gap(cell)
            jumps[f, pl.ds(cell, 8, stride=ny), :] = after - before
            before = after
        return carry

    lax.fori_loop(0, 5, y_field, 0, unroll=True)

    @pl.when(peers.last)
    def _():
        right_edge()

    def finish(part, f, cell, total):
        done_register[part, f, cell] = total
        state = xpad[f, pl.ds((cell + 3) * ny + part * 8, 8), :]
        done_state[part, f, cell] = state + UPDATE_WEIGHT * total

    def x_field(f, carry):
        turned = acc_t[f].T
        for part in range(parts):
            gap = prepared_gaps(alpha[0], lambda k, j: near[part, k, f, j - 1])
            for cell in range(cx):
                first = cell * ny + part * 8
                where = pl.ds(first, 8)
                jump = jumps[f, where, :] + turned[first : first + 8]
                if cell >= 2:
                    jump = jump + gap(cell)
                if cell >= 3:
                    finish(part, f, cell, acc[f, where, :] - mask[where, :] * (jump - gap(cell - 1)))
                else:
                    jumps[f, where, :] = jump
        return carry

    lax.fori_loop(0, 5, x_field, 0, unroll=True)

    for part in range(parts):
        to_right[part].wait_recv()
        if part < parts - 1:
            store_x_fluxes(ny, part, range(-3, 0), xpad, xf)
            flux = lambda f, j: xf[part, f, j + 3]
            known = lambda k, f, j: near[part, k, f, j - 1]
            emit = functools.partial(finish, part)
            left_edge(ny, part, alpha[0], xpad, flux, mask, acc, known, jumps, emit)
    for copy in to_left + to_right:
        copy.wait_send()

    def departures(plane):
        @pl.when(plane > peers.q)
        def _():
            all_of(plane, 1, send_sem)

        @pl.when(plane < peers.q)
        def _():
            all_of(plane, peers.members, send_sem)

    each(peers.planes, departures, peers.unroll)
    all_of(peers.q, peers.members - 1, send_sem)


def update_kernel(
    cx, ny, acc, xpad, mask, top_ref, edge_flux, edge_near, jumps, done_register, done_state,
    state_out, register_out, late_register, late_state, sems
):
    last = ny // 8 - 1
    copies = []

    def put(src, dst):
        copy = pltpu.make_async_copy(src, dst, sems.at[len(copies)])
        copy.start()
        copies.append(copy)

    for part in range(last + 1):
        first = 3 if part == last else 0
        block = pl.ds(first, cx - first)
        rows = pl.ds(part * 8, 8)
        put(done_register.at[part, :, block], register_out.at[:, block, rows, :])
        put(done_state.at[part, :, block], state_out.at[:, block, rows, :])
    halo = [
        fluxes_of([xpad[f, pl.ds((3 + cell) * ny + last * 8, 8), :] for f in range(5)], 1)
        for cell in range(-3, 0)
    ]

    def emit(f, cell, total):
        state = xpad[f, pl.ds((3 + cell) * ny + last * 8, 8), :]
        late_register[f, cell] = total
        late_state[f, cell] = state + UPDATE_WEIGHT * total

    alpha = jnp.broadcast_to(top_ref[:, 0:1], (8, 128))
    flux = lambda f, j: halo[j + 3][f] if j < 0 else edge_flux[f, j]
    known = lambda k, f, j: edge_near[k, f, j - 1]
    left_edge(ny, last, alpha, xpad, flux, mask, acc, known, jumps, emit)
    block, rows = pl.ds(0, 3), pl.ds(last * 8, 8)
    put(late_register, register_out.at[:, block, rows, :])
    put(late_state, state_out.at[:, block, rows, :])
    for copy in copies:
        copy.wait()


def shards(ngx, ngz, state, register, top_ghost, flags):
    _, cx, ny, cz = state.shape
    rows = cx * ny
    parts = ny // 8
    wide = plane_size(ngx)
    f32 = jnp.float32
    flat = lambda array: array.reshape(5, rows, cz)
    anywhere = pl.BlockSpec(memory_space=pl.ANY)
    inside = pl.BlockSpec(memory_space=pltpu.VMEM)
    held = pl.pallas_call(
        functools.partial(exchange_kernel, ngx, ngz, cx, ny),
        out_shape=(
            pltpu.VMEM((5, rows, cz), f32),
            pltpu.VMEM((5, (cx + 6) * ny, cz), f32),
            pltpu.VMEM((rows, cz), f32),
            pltpu.VMEM((8, 128), f32),
            pltpu.VMEM((5, 5, 8, cz), f32),
            pltpu.VMEM((11, 5, 3, 8, cz), f32),
            pltpu.VMEM((5, rows, cz), f32),
            pltpu.VMEM((parts, 5, cx, 8, cz), f32),
            pltpu.VMEM((parts, 5, cx, 8, cz), f32),
        ),
        in_specs=[anywhere] * 4,
        out_specs=(inside,) * 9,
        scratch_shapes=[
            pltpu.VMEM((5, cz + 16, rows), f32),
            pltpu.VMEM((5, rows, cz), f32),
            pltpu.VMEM((5, 3, cx, cz), f32),
            pltpu.VMEM((cx, 1, ny), jnp.int32),
            pltpu.VMEM((ngx // wide, wide * ngz, 1, 128), f32),
            pltpu.VMEM((1, 128), f32),
            pltpu.VMEM((1, 128), f32),
            pltpu.VMEM((5, cz, rows), f32),
            pltpu.VMEM((5, cz // 8 + 6, 8, rows), f32),
            pltpu.VMEM((5, cz // 8 + 6, 8, rows), f32),
            pltpu.VMEM((5, ny + 6, cx, cz), f32),
            pltpu.VMEM((5, ny + 6, cx, cz), f32),
            pltpu.VMEM((11, 5, ny + 4, cx, cz), f32),
            pltpu.VMEM((11, 5, cz // 8 + 4, 8, rows), f32),
            pltpu.VMEM((parts, 5, cx + 6, 8, cz), f32),
            pltpu.VMEM((parts, 11, 5, cx + 1, 8, cz), f32),
            pltpu.SemaphoreType.DMA,
            pltpu.SemaphoreType.DMA((3,)),
            pltpu.SemaphoreType.DMA((ngx // wide,)),
            pltpu.SemaphoreType.DMA((ngx // wide,)),
            pltpu.SemaphoreType.DMA((2 + 2 * parts,)),
            pltpu.SemaphoreType.DMA((2 + 2 * parts,)),
            pltpu.SemaphoreType.REGULAR((ngx // wide,)),
            pltpu.SemaphoreType.REGULAR,
        ],
        compiler_params=pltpu.CompilerParams(collective_id=0, has_side_effects=True),
        name="exchange",
    )(flat(state), flat(register), top_ghost.transpose(0, 2, 1, 3), flags.transpose(0, 2, 1))
    block = jax.ShapeDtypeStruct(state.shape, f32)
    return pl.pallas_call(
        functools.partial(update_kernel, cx, ny),
        out_shape=(block, block),
        in_specs=[inside] * 9,
        out_specs=(anywhere, anywhere),
        scratch_shapes=[
            pltpu.VMEM((5, 3, 8, cz), f32),
            pltpu.VMEM((5, 3, 8, cz), f32),
            pltpu.SemaphoreType.DMA((2 * parts + 2,)),
        ],
        name="update",
    )(*(pltpu.with_memory_space_constraint(array, pltpu.VMEM) for array in held))


def solution(mesh):
    block = P(None, "gx", None, "gz")
    return jax.shard_map(
        functools.partial(shards, mesh.shape["gx"], mesh.shape["gz"]),
        mesh=mesh,
        in_specs=(block, block, block, P("gx", None, "gz")),
        out_specs=(block, block),
        check_vma=False,
    )
```

```python
import functools

import jax
import jax.numpy as jnp
from jax import lax
from jax.experimental import pallas as pl
from jax.experimental.pallas import tpu as pltpu
from jax.sharding import PartitionSpec as P

MESH = pl.DeviceIdType.MESH
GAMMA = 1.4
EPS_WENO = 1e-06
LAMBDA = (0.1, 0.15, 0.1)
REGISTER_DECAY = -5.0 / 9.0
UPDATE_WEIGHT = 15.0 / 16.0
UNROLL_LIMIT = 64
MID = 6.0**-0.5


def reciprocal(value):
    return pltpu.reciprocal(value, approx=False)


def pressure_velocity(cons):
    inverse = reciprocal(cons[0])
    vel = [cons[1] * inverse, cons[2] * inverse, cons[3] * inverse]
    pressure = (GAMMA - 1.0) * (
        cons[4] - 0.5 * (cons[1] * vel[0] + cons[2] * vel[1] + cons[3] * vel[2])
    )
    return inverse, vel, pressure


def shifted(me, step, count):
    moved = me + step
    return jnp.where(moved >= count, moved - count, moved)


def each(count, action, unroll):
    if unroll:
        for index in range(count):
            action(index)
    else:
        def body(index, carry):
            action(index)
            return carry
        lax.fori_loop(0, count, body, 0)


def plane_size(ngx):
    return max(p for p in range(1, ngx + 1) if ngx % p == 0 and p * p <= ngx)


class Peers:
    def __init__(self, ngx, ngz):
        self.ngx, self.ngz = ngx, ngz
        self.gx, self.gz = lax.axis_index("gx"), lax.axis_index("gz")
        self.wide = plane_size(ngx)
        self.planes = ngx // self.wide
        self.members = self.wide * ngz
        self.q, self.r = lax.div(self.gx, self.wide), lax.rem(self.gx, self.wide)
        self.own = self.r * ngz + self.gz
        self.last = self.gx == ngx - 1
        self.unroll = self.planes * self.members < UNROLL_LIMIT

    def member(self, plane, index):
        if isinstance(index, int):
            return plane * self.wide + index // self.ngz, index % self.ngz
        return plane * self.wide + lax.div(index, self.ngz), lax.rem(index, self.ngz)

    def plane_mates(self, action):
        def visit(index):
            @pl.when(self.own != index)
            def _():
                action(index, *self.member(self.q, index))
        each(self.members, visit, self.unroll)

    def of_planes(self, wanted, action):
        def visit(plane):
            @pl.when(wanted(plane))
            def _():
                each(self.members, lambda index: action(index, *self.member(plane, index)), self.unroll)
        each(self.planes, visit, self.unroll)

    def columns(self, wanted, action):
        def visit(plane):
            @pl.when(wanted(plane))
            def _():
                action(plane, (plane * self.wide + self.r, self.gz))
        each(self.planes, visit, self.unroll)

    def greet(self, barrier):
        def signal(tx, tz):
            pl.semaphore_signal(barrier, inc=1, device_id=(tx, tz), device_id_type=MESH)

        @pl.when((self.r == 0) & (self.gx > 0))
        def _():
            signal(self.gx - 1, self.gz)

        self.plane_mates(lambda index, tx, tz: signal(tx, tz))
        self.of_planes(lambda plane: plane > self.q, lambda index, tx, tz: signal(tx, tz))

    def greetings(self):
        has_next = (self.r == self.wide - 1) & jnp.logical_not(self.last)
        return self.members - 1 + self.q * self.members + has_next.astype(jnp.int32)


def cached(function):
    return functools.lru_cache(None)(function)


class Line:
    def __init__(self, load):
        self.load = cached(load)
        self.D = cached(lambda j: self.load(j + 1) - self.load(j))
        self.S = cached(lambda j: self.D(j) - self.D(j - 1))
        self.T = cached(lambda j: self.S(j + 1) - self.S(j))
        self.S2 = cached(lambda j: self.S(j) + self.S(j))
        self.C = cached(
            lambda j: (self.S(j) * self.S(j) * (4.0 / 3.0) + 4.0 * EPS_WENO)
            + self.D(j) * self.D(j - 1)
        )
        self.L = cached(lambda j: self.C(j) + self.S2(j) * self.D(j))
        self.M = cached(lambda j: MID * self.C(j))
        self.R = cached(lambda j: self.C(j) - self.S2(j) * self.D(j - 1))


def correction(near, mid, far, t_near, t_far):
    a, b, c = mid * far, near * far, near * mid
    w_near = a * a
    w_far = 3.0 * (c * c)
    total = w_near + b * b + w_far
    return (w_far * t_far + (w_near + w_near) * t_near) * reciprocal(total)


def face_gap(plus, minus, drift_t):
    def gap(j):
        up = correction(plus.L(j - 1), plus.M(j), plus.R(j + 1), plus.T(j - 1), plus.T(j))
        down = correction(minus.R(j + 2), minus.M(j + 1), minus.L(j), minus.T(j + 1), minus.T(j))
        return drift_t(j) - up + down

    return gap


KINDS = ("L", "M", "R")


def prepare(flux, cons, cells, store):
    f, u = Line(flux), Line(cons)
    for j in cells:
        mixed = (8.0 / 3.0) * (f.S(j) * u.S(j)) + (f.D(j) * u.D(j - 1) + f.D(j - 1) * u.D(j))
        curved = (4.0 / 3.0) * (u.S(j) * u.S(j)) + u.D(j) * u.D(j - 1)
        centre = (f.C(j), mixed, curved)

        def product(at):
            return (
                f.S2(j) * f.D(at),
                f.S2(j) * u.D(at) + u.S2(j) * f.D(at),
                u.S2(j) * u.D(at),
            )

        left = [c + p for c, p in zip(centre, product(j))]
        right = [c - p for c, p in zip(centre, product(j - 1))]
        for kind, terms in enumerate((left, [MID * c for c in centre], right)):
            for power, term in enumerate(terms):
                store(3 * kind + power, j, term)


def prepare_third(flux, cons, cells, store, scale=1.0):
    f, u = Line(flux), Line(cons)
    for j in cells:
        store(9, j, f.T(j) if scale == 1.0 else scale * f.T(j))
        store(10, j, u.T(j) if scale == 1.0 else scale * u.T(j))


class Prepared:
    def __init__(self, alpha, load):
        square = alpha * alpha

        def both(kind):
            def pair(j):
                even = load(3 * kind, j) + square * load(3 * kind + 2, j)
                odd = alpha * load(3 * kind + 1, j)
                return even + odd, even - odd
            return cached(pair)

        self.drift_t = cached(lambda j: alpha * load(10, j))
        third = cached(lambda j: (load(9, j) + self.drift_t(j), load(9, j) - self.drift_t(j)))
        pairs = {name: both(kind) for kind, name in enumerate(KINDS)} | {"T": third}
        self.side = [
            {name: (lambda j, pair=pair, k=k: pair(j)[k]) for name, pair in pairs.items()} for k in range(2)
        ]


class Side:
    def __init__(self, values):
        self.L, self.M, self.R, self.T = (values[name] for name in (*KINDS, "T"))


def prepared_gaps(alpha, load):
    ready = Prepared(alpha, load)
    return face_gap(Side(ready.side[0]), Side(ready.side[1]), ready.drift_t)


def edge_gaps(alpha, load_flux, load_cons, load, inner, inner_t):
    flux = cached(load_flux)
    drift = cached(lambda j: alpha * load_cons(j))
    ready = Prepared(alpha, load)
    fresh = Line(lambda j: flux(j) + drift(j)), Line(lambda j: flux(j) - drift(j))

    def mixed(k):
        def pick(name):
            known = inner_t if name == "T" else inner
            return lambda j: ready.side[k][name](j) if j in known else getattr(fresh[k], name)(j)
        return Side({name: pick(name) for name in (*KINDS, "T")})

    plus, minus = mixed(0), mixed(1)

    def drift_t(j):
        return ready.drift_t(j) if j in inner_t else 0.5 * (plus.T(j) - minus.T(j))

    return face_gap(plus, minus, drift_t)


def difference_weights(flagged):
    return (
        jnp.where(flagged, 8.0, 9.0),
        jnp.where(flagged, -1.0, -1.8),
        jnp.where(flagged, 0.0, 0.2),
    )


def linear_part(weights, flux, cell):
    total = None
    for reach, weight in enumerate(weights, 1):
        high, low = flux(cell + reach), flux(cell - reach)
        if high is None and low is None:
            continue
        gap = -low if high is None else high if low is None else high - low
        total = weight * gap if total is None else total + weight * gap
    return total


def fluxes_of(cons, var):
    _, vel, pressure = pressure_velocity(cons)
    velocity = vel[var - 1]
    fluxes = [cons[field] * velocity for field in range(4)]
    fluxes.append((cons[4] + pressure) * velocity)
    fluxes[var] = fluxes[var] + pressure
    return fluxes


def store_fluxes(cons, var, fluxes, conserved, cell):
    for field, flux in enumerate(fluxes_of(cons, var)):
        fluxes[field, cell] = flux
        conserved[field, cell] = cons[field]


def prepare_line(count, scale, f, fluxes, conserved, out):
    def keep(kind, j, value):
        out[kind, f, j + 2] = value

    flux, cons = cached(lambda j: fluxes[f, j + 3]), cached(lambda j: conserved[f, j + 3])
    prepare(flux, cons, range(-2, count + 2), keep)
    prepare_third(flux, cons, range(-2, count + 1), keep, scale)


def store_x_fluxes(ny, part, cells, xpad, xf):
    for cell in cells:
        cons = [xpad[f, pl.ds((cell + 3) * ny + part * 8, 8), :] for f in range(5)]
        for field, flux in enumerate(fluxes_of(cons, 1)):
            xf[part, field, cell + 3] = flux


def left_edge(ny, part, alpha, xpad, flux, mask, acc, known, jumps, emit):
    rows = lambda cell: pl.ds(cell * ny + part * 8, 8)
    scaled = [mask[rows(cell), :] for cell in range(3)]
    weights = [
        [weight * (LAMBDA[0] / 12.0) for weight in difference_weights(m > 0.0)] for m in scaled
    ]
    for f in range(5):
        gap = edge_gaps(
            alpha, lambda j: flux(f, j), lambda j: xpad[f, rows(j + 3), :],
            lambda k, j: known(k, f, j), range(1, 4), range(1, 4),
        )
        outside = lambda j: flux(f, j) if j < 0 else None
        for cell in range(3):
            jump = jumps[f, rows(cell), :] - gap(cell - 1)
            if cell < 2:
                jump = jump + gap(cell)
            missing = linear_part(weights[cell], outside, cell)
            emit(f, cell, acc[f, rows(cell), :] - (missing + scaled[cell] * jump))


def exchange_kernel(
    ngx, ngz, cx, ny, state_ref, register_ref, ghost_ref, flags_ref,
    acc, xpad, mask, top_ref, edge_flux, edge_near, jumps, done_register, done_state,
    zt, reg, ghost, flags, slots, mine, plane_top, acc_t, zf, zu, yf, yu, yq, zq, xf, near,
    load_sem, side_sem, send_sem, recv_sem, halo_send, halo_recv, ready_up, ready_wrap
):
    peers = Peers(ngx, ngz)
    gx, gz = peers.gx, peers.gz
    parts = ny // 8
    rows = cx * ny
    halo = 3 * ny
    strip = zt.shape[1] - 16
    chunk = strip // 8
    load = pltpu.make_async_copy(state_ref, xpad.at[:, pl.ds(halo, rows), :], load_sem)
    load.start()
    load_flags = pltpu.make_async_copy(flags_ref, flags, side_sem.at[0])
    load_ghost = pltpu.make_async_copy(ghost_ref, ghost, side_sem.at[1])
    load_register = pltpu.make_async_copy(register_ref, reg, load_sem)
    slots[...] = jnp.zeros(slots.shape, slots.dtype)
    barrier = pltpu.get_barrier_semaphore()
    peers.greet(barrier)
    load.wait()
    load_flags.start()
    load_ghost.start()
    load_register.start()
    best = None
    for row in range(0, rows, 8):
        cons = [xpad[var, pl.ds(halo + row, 8), :] for var in range(5)]
        inverse, vel, pressure = pressure_velocity(cons)
        sound = jnp.sqrt(GAMMA * pressure * inverse)
        local = [jnp.abs(v) + sound for v in vel]
        best = local if best is None else [jnp.maximum(a, b) for a, b in zip(best, local)]
    tops = [jnp.max(jnp.max(b, axis=0, keepdims=True), axis=1, keepdims=True) for b in best]
    lane = lax.broadcasted_iota(jnp.int32, (1, 128), 1)
    mine[...] = jnp.where(lane == 0, tops[0], jnp.where(lane == 1, tops[1], tops[2]))

    right, left = shifted(gx, 1, ngx), shifted(gx, ngx - 1, ngx)
    high, low = shifted(gz, 1, ngz), shifted(gz, ngz - 1, ngz)

    def move(leaves, comes, src, dst, target):
        return pltpu.make_async_remote_copy(
            src_ref=src, dst_ref=dst, send_sem=halo_send.at[leaves], recv_sem=halo_recv.at[comes],
            device_id=target, device_id_type=MESH,
        )

    def all_bytes(some, semaphore):
        pltpu.make_async_copy(some, some, semaphore).wait()

    blocks = xpad.reshape(5, cx + 6, ny, xpad.shape[2])
    to_left, to_right = [], []
    for part in range(parts):
        layers = lambda first: blocks.at[:, pl.ds(first, 3), pl.ds(part * 8, 8), :]
        to_left.append(move(1, 1, layers(3), layers(3 + cx), (left, gz)))
        to_right.append(move(1, 2 + part, layers(cx), layers(0), (right, gz)))

    def start(copies):
        for copy in copies:
            copy.start()

    def signal(semaphore, target):
        pl.semaphore_signal(semaphore, inc=1, device_id=target, device_id_type=MESH)

    def tell(source, far, index, target):
        pltpu.make_async_remote_copy(
            src_ref=source, dst_ref=slots.at[peers.q, index], send_sem=send_sem,
            recv_sem=recv_sem.at[far], device_id=target, device_id_type=MESH,
        ).start()

    pl.semaphore_wait(barrier, peers.greetings())

    def tell_lower(plane):
        @pl.when(plane < peers.q)
        def _():
            each(
                peers.members,
                lambda index: tell(mine, 1, peers.own, peers.member(plane, index)),
                peers.unroll,
            )

    each(peers.planes, tell_lower, peers.unroll)
    peers.plane_mates(lambda index, tx, tz: tell(mine, 0, peers.own, (tx, tz)))

    yields = peers.last & (gz > 0)

    @pl.when(peers.last)
    def _():
        signal(ready_wrap, (0, gz))
        start(to_right[:1])

    @pl.when(peers.last & (gz == 0))
    def _():
        start(to_right[1:])

    @pl.when((gx > 0) & jnp.logical_not(yields))
    def _():
        start(to_left)

    @pl.when(jnp.logical_not(peers.last))
    def _():
        start(to_right)

    peers.columns(lambda plane: plane < peers.q, lambda plane, target: signal(ready_up, target))
    for var in range(5):
        zt[var, pl.ds(8, strip), :] = xpad[var, pl.ds(halo, rows), :].T
    z_copies = [
        move(0, 0, zt.at[:, pl.ds(8, 8), :], zt.at[:, pl.ds(8 + strip, 8), :], (gx, low)),
        move(0, 0, zt.at[:, pl.ds(strip, 8), :], zt.at[:, pl.ds(0, 8), :], (gx, high)),
    ]
    start(z_copies)
    load_flags.wait()
    for x in range(cx):
        wide = jnp.broadcast_to(flags[x], (strip, ny)).astype(jnp.float32).T * (LAMBDA[0] / 12.0)
        mask[pl.ds(x * ny, ny), :] = wide
    mask_t = mask[...].T[:8]
    flag_t = mask_t > 0.0

    load_ghost.wait()
    for cell in range(ny + 6):
        y = cell - 3
        if y < ny:
            source = y if y >= 0 else -1 - y
            cons = [xpad[f, pl.ds(halo + source, 8, stride=ny), :] for f in range(5)]
            if y < 0:
                cons[2] = -cons[2]
        else:
            cons = [ghost[f, y - ny] for f in range(5)]
        store_fluxes(cons, 2, yf, yu, cell)
    load_register.wait()

    def y_linear(f, carry):
        for cell in range(ny):
            where = pl.ds(cell, 8, stride=ny)
            weights = difference_weights(mask[where, :] > 0.0)
            linear = linear_part(weights, lambda j: yf[f, j + 3], cell)
            acc[f, where, :] = REGISTER_DECAY * reg[f, where, :] - (LAMBDA[1] / 12.0) * linear
        prepare_line(ny, LAMBDA[1] / LAMBDA[0], f, yf, yu, yq)
        return carry

    lax.fori_loop(0, 5, y_linear, 0)

    @pl.when(yields)
    def _():
        start(to_right[1:])
        start(to_left)

    for part in range(parts):
        store_x_fluxes(ny, part, range(cx), xpad, xf)

    def x_prepare(f, part, centres, thirds):
        def keep(kind, j, value):
            near[part, kind, f, j - 1] = value

        flux = cached(lambda j: xf[part, f, j + 3])
        cons = cached(lambda j: xpad[f, pl.ds((j + 3) * ny + part * 8, 8), :])
        prepare(flux, cons, centres, keep)
        prepare_third(flux, cons, thirds, keep)

    def x_linear(f, part, cells, known):
        for cell in cells:
            where = pl.ds(cell * ny + part * 8, 8)
            weights = difference_weights(mask[where, :] > 0.0)
            linear = linear_part(weights, lambda j: xf[part, f, j + 3] if known(j) else None, cell)
            acc[f, where, :] = acc[f, where, :] - (LAMBDA[0] / 12.0) * linear

    def x_inner(f, carry):
        for part in range(parts):
            x_prepare(f, part, range(1, cx - 1), range(1, cx - 2))
            if part == parts - 1:
                for cell in range(5):
                    edge_flux[f, cell] = xf[part, f, cell + 3]
                for kind in range(11):
                    for j in range(1, 4):
                        edge_near[kind, f, j - 1] = near[part, kind, f, j - 1]
            x_linear(f, part, range(cx), lambda j: 0 <= j < cx)
        return carry

    lax.fori_loop(0, 5, x_inner, 0)

    def right_edge():
        all_bytes(xpad.at[:, pl.ds(0, halo), :], halo_recv.at[1])
        for part in range(parts):
            store_x_fluxes(ny, part, range(cx, cx + 3), xpad, xf)

        def field(f, carry):
            for part in range(parts):
                x_prepare(f, part, range(cx - 1, cx + 2), range(cx - 2, cx + 1))
                x_linear(f, part, range(cx - 3, cx), lambda j: j >= cx)
            return carry

        lax.fori_loop(0, 5, field, 0)

    all_bytes(zt.at[:, pl.ds(0, 16), :], halo_send.at[0])
    all_bytes(zt.at[:, pl.ds(0, 16), :], halo_recv.at[0])
    for cell in range(chunk + 6):
        cons = [zt[f, pl.ds(5 + cell, 8, stride=chunk), :] for f in range(5)]
        store_fluxes(cons, 3, zf, zu, cell)
    weights_t = [w * (-LAMBDA[2] / 12.0) for w in difference_weights(flag_t)]

    def z_linear(f, carry):
        for cell in range(chunk):
            linear = linear_part(weights_t, lambda j: zf[f, j + 3], cell)
            acc_t[f, pl.ds(cell, 8, stride=chunk), :] = linear
        acc[f] = acc[f] + acc_t[f].T
        prepare_line(chunk, LAMBDA[2] / LAMBDA[0], f, zf, zu, zq)
        return carry

    lax.fori_loop(0, 5, z_linear, 0)

    messages = slots.reshape(peers.planes * peers.members, 1, 128)

    def by_plane(count, semaphore):
        def visit(plane):
            number = count(plane)
            if number:
                @pl.when(peers.q == plane)
                def _():
                    all_bytes(messages.at[pl.ds(0, number)], semaphore)

        for plane in range(peers.planes):
            visit(plane)

    all_bytes(messages.at[pl.ds(0, peers.members - 1)], recv_sem.at[0])
    plane_top[...] = jnp.maximum(jnp.max(slots[peers.q], axis=0), mine[...])

    @pl.when(peers.q < peers.planes - 1)
    def _():
        pl.semaphore_wait(ready_up, peers.planes - 1 - peers.q)

    peers.columns(lambda plane: plane > peers.q, lambda plane, target: tell(plane_top, 1, 0, target))

    @pl.when(gx == 0)
    def _():
        pl.semaphore_wait(ready_wrap, 1)
        start(to_left)

    @pl.when(jnp.logical_not(peers.last))
    def _():
        right_edge()

    by_plane(lambda plane: (peers.planes - 1 - plane) * peers.members + plane, recv_sem.at[1])
    top = jnp.maximum(jnp.max(jnp.max(slots[...], axis=0), axis=0), mine[...])
    top_ref[...] = jnp.broadcast_to(top, (8, 128))
    alpha = [jnp.broadcast_to(top[:, k : k + 1], (8, 128)) for k in range(3)]

    def z_field(f, carry):
        gap = prepared_gaps(alpha[2], lambda k, j: zq[k, f, j + 2])
        before = gap(-1)
        for cell in range(chunk):
            after = gap(cell)
            acc_t[f, pl.ds(cell, 8, stride=chunk), :] = after - before
            before = after
        return carry

    lax.fori_loop(0, 5, z_field, 0, unroll=True)

    def y_field(f):
        gap = prepared_gaps(alpha[1], lambda k, j: yq[k, f, j + 2])
        before = gap(-1) if f == 2 else None
        for cell in range(ny):
            after = gap(cell)
            jumps[f, pl.ds(cell, 8, stride=ny), :] = after if before is None else after - before
            before = after

    for f in range(5):
        y_field(f)

    @pl.when(peers.last)
    def _():
        right_edge()

    def finish(part, f, cell, total):
        done_register[part, f, cell] = total
        state = xpad[f, pl.ds((cell + 3) * ny + part * 8, 8), :]
        done_state[part, f, cell] = state + UPDATE_WEIGHT * total

    def x_field(f, carry):
        turned = acc_t[f].T
        for part in range(parts):
            gap = prepared_gaps(alpha[0], lambda k, j: near[part, k, f, j - 1])
            for cell in range(cx):
                first = cell * ny + part * 8
                where = pl.ds(first, 8)
                jump = jumps[f, where, :] + turned[first : first + 8]
                if cell >= 2:
                    jump = jump + gap(cell)
                if cell >= 3:
                    finish(part, f, cell, acc[f, where, :] - mask[where, :] * (jump - gap(cell - 1)))
                else:
                    jumps[f, where, :] = jump
        return carry

    lax.fori_loop(0, 5, x_field, 0, unroll=True)

    for part in range(parts):
        to_right[part].wait_recv()
        if part < parts - 1:
            store_x_fluxes(ny, part, range(-3, 0), xpad, xf)
            flux = lambda f, j: xf[part, f, j + 3]
            known = lambda k, f, j: near[part, k, f, j - 1]
            emit = functools.partial(finish, part)
            left_edge(ny, part, alpha[0], xpad, flux, mask, acc, known, jumps, emit)
    all_bytes(xpad.at[:, pl.ds(0, 2 * halo), :], halo_send.at[1])

    by_plane(lambda plane: (plane + 1) * peers.members - 1 + peers.planes - 1 - plane, send_sem)


def update_kernel(
    cx, ny, acc, xpad, mask, top_ref, edge_flux, edge_near, jumps, done_register, done_state,
    state_out, register_out, late_register, late_state, sems
):
    last = ny // 8 - 1

    def put(src, dst, which):
        pltpu.make_async_copy(src, dst, sems.at[which]).start()

    for part in range(last + 1):
        first = 3 if part == last else 0
        block = pl.ds(first, cx - first)
        rows = pl.ds(part * 8, 8)
        put(done_register.at[part, :, block], register_out.at[:, block, rows, :], 0)
        put(done_state.at[part, :, block], state_out.at[:, block, rows, :], 1)
    halo = [
        fluxes_of([xpad[f, pl.ds((3 + cell) * ny + last * 8, 8), :] for f in range(5)], 1)
        for cell in range(-3, 0)
    ]

    def emit(f, cell, total):
        state = xpad[f, pl.ds((3 + cell) * ny + last * 8, 8), :]
        late_register[f, cell] = total
        late_state[f, cell] = state + UPDATE_WEIGHT * total

    alpha = jnp.broadcast_to(top_ref[:, 0:1], (8, 128))
    flux = lambda f, j: halo[j + 3][f] if j < 0 else edge_flux[f, j]
    known = lambda k, f, j: edge_near[k, f, j - 1]
    left_edge(ny, last, alpha, xpad, flux, mask, acc, known, jumps, emit)
    block, rows = pl.ds(0, 3), pl.ds(last * 8, 8)
    put(late_register, register_out.at[:, block, rows, :], 0)
    put(late_state, state_out.at[:, block, rows, :], 1)
    for which, out in enumerate((register_out, state_out)):
        pltpu.make_async_copy(out, out, sems.at[which]).wait()


def shards(ngx, ngz, state, register, top_ghost, flags):
    _, cx, ny, cz = state.shape
    rows = cx * ny
    parts = ny // 8
    wide = plane_size(ngx)
    f32 = jnp.float32
    flat = lambda array: array.reshape(5, rows, cz)
    anywhere = pl.BlockSpec(memory_space=pl.ANY)
    inside = pl.BlockSpec(memory_space=pltpu.VMEM)
    held = pl.pallas_call(
        functools.partial(exchange_kernel, ngx, ngz, cx, ny),
        out_shape=(
            pltpu.VMEM((5, rows, cz), f32),
            pltpu.VMEM((5, (cx + 6) * ny, cz), f32),
            pltpu.VMEM((rows, cz), f32),
            pltpu.VMEM((8, 128), f32),
            pltpu.VMEM((5, 5, 8, cz), f32),
            pltpu.VMEM((11, 5, 3, 8, cz), f32),
            pltpu.VMEM((5, rows, cz), f32),
            pltpu.VMEM((parts, 5, cx, 8, cz), f32),
            pltpu.VMEM((parts, 5, cx, 8, cz), f32),
        ),
        in_specs=[anywhere] * 4,
        out_specs=(inside,) * 9,
        scratch_shapes=[
            pltpu.VMEM((5, cz + 16, rows), f32),
            pltpu.VMEM((5, rows, cz), f32),
            pltpu.VMEM((5, 3, cx, cz), f32),
            pltpu.VMEM((cx, 1, ny), jnp.int32),
            pltpu.VMEM((ngx // wide, wide * ngz, 1, 128), f32),
            pltpu.VMEM((1, 128), f32),
            pltpu.VMEM((1, 128), f32),
            pltpu.VMEM((5, cz, rows), f32),
            pltpu.VMEM((5, cz // 8 + 6, 8, rows), f32),
            pltpu.VMEM((5, cz // 8 + 6, 8, rows), f32),
            pltpu.VMEM((5, ny + 6, cx, cz), f32),
            pltpu.VMEM((5, ny + 6, cx, cz), f32),
            pltpu.VMEM((11, 5, ny + 4, cx, cz), f32),
            pltpu.VMEM((11, 5, cz // 8 + 4, 8, rows), f32),
            pltpu.VMEM((parts, 5, cx + 6, 8, cz), f32),
            pltpu.VMEM((parts, 11, 5, cx + 1, 8, cz), f32),
            pltpu.SemaphoreType.DMA,
            pltpu.SemaphoreType.DMA((2,)),
            pltpu.SemaphoreType.DMA,
            pltpu.SemaphoreType.DMA((2,)),
            pltpu.SemaphoreType.DMA((2,)),
            pltpu.SemaphoreType.DMA((2 + parts,)),
            pltpu.SemaphoreType.REGULAR,
            pltpu.SemaphoreType.REGULAR,
        ],
        compiler_params=pltpu.CompilerParams(collective_id=0, has_side_effects=True),
        name="exchange",
    )(flat(state), flat(register), top_ghost.transpose(0, 2, 1, 3), flags.transpose(0, 2, 1))
    block = jax.ShapeDtypeStruct(state.shape, f32)
    return pl.pallas_call(
        functools.partial(update_kernel, cx, ny),
        out_shape=(block, block),
        in_specs=[inside] * 9,
        out_specs=(anywhere, anywhere),
        scratch_shapes=[
            pltpu.VMEM((5, 3, 8, cz), f32),
            pltpu.VMEM((5, 3, 8, cz), f32),
            pltpu.SemaphoreType.DMA((2,)),
        ],
        name="update",
    )(*(pltpu.with_memory_space_constraint(array, pltpu.VMEM) for array in held))


def solution(mesh):
    block = P(None, "gx", None, "gz")
    return jax.shard_map(
        functools.partial(shards, mesh.shape["gx"], mesh.shape["gz"]),
        mesh=mesh,
        in_specs=(block, block, block, P("gx", None, "gz")),
        out_specs=(block, block),
        check_vma=False,
    )
```

```python
import functools

import jax
import jax.numpy as jnp
from jax import lax
from jax.experimental import pallas as pl
from jax.experimental.pallas import tpu as pltpu
from jax.sharding import PartitionSpec as P

MESH = pl.DeviceIdType.MESH
GAMMA = 1.4
EPS_WENO = 1e-06
LAMBDA = (0.1, 0.15, 0.1)
REGISTER_DECAY = -5.0 / 9.0
UPDATE_WEIGHT = 15.0 / 16.0
UNROLL_LIMIT = 64
MID = 6.0**-0.5


def reciprocal(value):
    return pltpu.reciprocal(value, approx=False)


def pressure_velocity(cons):
    inverse = reciprocal(cons[0])
    vel = [cons[1] * inverse, cons[2] * inverse, cons[3] * inverse]
    pressure = (GAMMA - 1.0) * (
        cons[4] - 0.5 * (cons[1] * vel[0] + cons[2] * vel[1] + cons[3] * vel[2])
    )
    return inverse, vel, pressure


def shifted(me, step, count):
    moved = me + step
    return jnp.where(moved >= count, moved - count, moved)


def each(count, action, unroll):
    if unroll:
        for index in range(count):
            action(index)
    else:
        def body(index, carry):
            action(index)
            return carry
        lax.fori_loop(0, count, body, 0)


def plane_size(ngx):
    return max(p for p in range(1, ngx + 1) if ngx % p == 0 and p * p <= ngx)


class Peers:
    def __init__(self, ngx, ngz):
        self.ngx, self.ngz = ngx, ngz
        self.gx, self.gz = lax.axis_index("gx"), lax.axis_index("gz")
        self.wide = plane_size(ngx)
        self.planes = ngx // self.wide
        self.members = self.wide * ngz
        self.q, self.r = lax.div(self.gx, self.wide), lax.rem(self.gx, self.wide)
        self.own = self.r * ngz + self.gz
        self.last = self.gx == ngx - 1
        self.unroll = self.planes * self.members < UNROLL_LIMIT

    def member(self, plane, index):
        if isinstance(index, int):
            return plane * self.wide + index // self.ngz, index % self.ngz
        return plane * self.wide + lax.div(index, self.ngz), lax.rem(index, self.ngz)

    def plane_mates(self, action):
        def visit(index):
            @pl.when(self.own != index)
            def _():
                action(index, *self.member(self.q, index))
        each(self.members, visit, self.unroll)

    def of_planes(self, wanted, action):
        def visit(plane):
            @pl.when(wanted(plane))
            def _():
                each(self.members, lambda index: action(index, *self.member(plane, index)), self.unroll)
        each(self.planes, visit, self.unroll)

    def columns(self, wanted, action):
        def visit(plane):
            @pl.when(wanted(plane))
            def _():
                action(plane, (plane * self.wide + self.r, self.gz))
        each(self.planes, visit, self.unroll)

    def greet(self, barrier):
        def signal(tx, tz):
            pl.semaphore_signal(barrier, inc=1, device_id=(tx, tz), device_id_type=MESH)

        @pl.when((self.r == 0) & (self.gx > 0))
        def _():
            signal(self.gx - 1, self.gz)

        self.plane_mates(lambda index, tx, tz: signal(tx, tz))
        self.of_planes(lambda plane: plane > self.q, lambda index, tx, tz: signal(tx, tz))

    def greetings(self):
        has_next = (self.r == self.wide - 1) & jnp.logical_not(self.last)
        return self.members - 1 + self.q * self.members + has_next.astype(jnp.int32)


def cached(function):
    return functools.lru_cache(None)(function)


class Line:
    def __init__(self, load):
        self.load = cached(load)
        self.D = cached(lambda j: self.load(j + 1) - self.load(j))
        self.S = cached(lambda j: self.D(j) - self.D(j - 1))
        self.T = cached(lambda j: self.S(j + 1) - self.S(j))
        self.S2 = cached(lambda j: self.S(j) + self.S(j))
        self.C = cached(
            lambda j: (self.S(j) * self.S(j) * (4.0 / 3.0) + 4.0 * EPS_WENO)
            + self.D(j) * self.D(j - 1)
        )
        self.L = cached(lambda j: self.C(j) + self.S2(j) * self.D(j))
        self.M = cached(lambda j: MID * self.C(j))
        self.R = cached(lambda j: self.C(j) - self.S2(j) * self.D(j - 1))


def correction(near, mid, far, t_near, t_far):
    a, b, c = mid * far, near * far, near * mid
    w_near = a * a
    w_far = 3.0 * (c * c)
    total = w_near + b * b + w_far
    return (w_far * t_far + (w_near + w_near) * t_near) * reciprocal(total)


def face_gap(plus, minus, drift_t):
    def gap(j):
        up = correction(plus.L(j - 1), plus.M(j), plus.R(j + 1), plus.T(j - 1), plus.T(j))
        down = correction(minus.R(j + 2), minus.M(j + 1), minus.L(j), minus.T(j + 1), minus.T(j))
        return drift_t(j) - up + down

    return gap


KINDS = ("L", "M", "R")


def prepare(flux, cons, cells, store):
    f, u = Line(flux), Line(cons)
    for j in cells:
        mixed = (8.0 / 3.0) * (f.S(j) * u.S(j)) + (f.D(j) * u.D(j - 1) + f.D(j - 1) * u.D(j))
        curved = (4.0 / 3.0) * (u.S(j) * u.S(j)) + u.D(j) * u.D(j - 1)
        centre = (f.C(j), mixed, curved)

        def product(at):
            return (
                f.S2(j) * f.D(at),
                f.S2(j) * u.D(at) + u.S2(j) * f.D(at),
                u.S2(j) * u.D(at),
            )

        left = [c + p for c, p in zip(centre, product(j))]
        right = [c - p for c, p in zip(centre, product(j - 1))]
        for kind, terms in enumerate((left, [MID * c for c in centre], right)):
            for power, term in enumerate(terms):
                store(3 * kind + power, j, term)


def prepare_third(flux, cons, cells, store, scale=1.0):
    f, u = Line(flux), Line(cons)
    for j in cells:
        store(9, j, f.T(j) if scale == 1.0 else scale * f.T(j))
        store(10, j, u.T(j) if scale == 1.0 else scale * u.T(j))


class Prepared:
    def __init__(self, alpha, load):
        square = alpha * alpha

        def both(kind):
            def pair(j):
                even = load(3 * kind, j) + square * load(3 * kind + 2, j)
                odd = alpha * load(3 * kind + 1, j)
                return even + odd, even - odd
            return cached(pair)

        self.drift_t = cached(lambda j: alpha * load(10, j))
        third = cached(lambda j: (load(9, j) + self.drift_t(j), load(9, j) - self.drift_t(j)))
        pairs = {name: both(kind) for kind, name in enumerate(KINDS)} | {"T": third}
        self.side = [
            {name: (lambda j, pair=pair, k=k: pair(j)[k]) for name, pair in pairs.items()} for k in range(2)
        ]


class Side:
    def __init__(self, values):
        self.L, self.M, self.R, self.T = (values[name] for name in (*KINDS, "T"))


def prepared_gaps(alpha, load):
    ready = Prepared(alpha, load)
    return face_gap(Side(ready.side[0]), Side(ready.side[1]), ready.drift_t)


def edge_gaps(alpha, load_flux, load_cons, load, inner, inner_t):
    flux = cached(load_flux)
    drift = cached(lambda j: alpha * load_cons(j))
    ready = Prepared(alpha, load)
    fresh = Line(lambda j: flux(j) + drift(j)), Line(lambda j: flux(j) - drift(j))

    def mixed(k):
        def pick(name):
            known = inner_t if name == "T" else inner
            return lambda j: ready.side[k][name](j) if j in known else getattr(fresh[k], name)(j)
        return Side({name: pick(name) for name in (*KINDS, "T")})

    plus, minus = mixed(0), mixed(1)

    def drift_t(j):
        return ready.drift_t(j) if j in inner_t else 0.5 * (plus.T(j) - minus.T(j))

    return face_gap(plus, minus, drift_t)


def difference_weights(flagged):
    return (
        jnp.where(flagged, 8.0, 9.0),
        jnp.where(flagged, -1.0, -1.8),
        jnp.where(flagged, 0.0, 0.2),
    )


def linear_part(weights, flux, cell):
    total = None
    for reach, weight in enumerate(weights, 1):
        high, low = flux(cell + reach), flux(cell - reach)
        if high is None and low is None:
            continue
        gap = -low if high is None else high if low is None else high - low
        total = weight * gap if total is None else total + weight * gap
    return total


def fluxes_of(cons, var):
    _, vel, pressure = pressure_velocity(cons)
    velocity = vel[var - 1]
    fluxes = [cons[field] * velocity for field in range(4)]
    fluxes.append((cons[4] + pressure) * velocity)
    fluxes[var] = fluxes[var] + pressure
    return fluxes


def store_fluxes(cons, var, fluxes, conserved, cell):
    for field, flux in enumerate(fluxes_of(cons, var)):
        fluxes[field, cell] = flux
        conserved[field, cell] = cons[field]


def prepare_line(count, scale, f, fluxes, conserved, out):
    def keep(kind, j, value):
        out[kind, f, j + 2] = value

    flux, cons = cached(lambda j: fluxes[f, j + 3]), cached(lambda j: conserved[f, j + 3])
    prepare(flux, cons, range(-2, count + 2), keep)
    prepare_third(flux, cons, range(-2, count + 1), keep, scale)


def store_x_fluxes(ny, part, cells, xpad, xf):
    for cell in cells:
        cons = [xpad[f, pl.ds((cell + 3) * ny + part * 8, 8), :] for f in range(5)]
        for field, flux in enumerate(fluxes_of(cons, 1)):
            xf[part, field, cell + 3] = flux


def left_edge(ny, part, alpha, xpad, flux, mask, acc, known, jumps, emit):
    rows = lambda cell: pl.ds(cell * ny + part * 8, 8)
    scaled = [mask[rows(cell), :] for cell in range(3)]
    weights = [
        [weight * (LAMBDA[0] / 12.0) for weight in difference_weights(m > 0.0)] for m in scaled
    ]
    for f in range(5):
        gap = edge_gaps(
            alpha, lambda j: flux(f, j), lambda j: xpad[f, rows(j + 3), :],
            lambda k, j: known(k, f, j), range(1, 4), range(1, 4),
        )
        outside = lambda j: flux(f, j) if j < 0 else None
        for cell in range(3):
            jump = jumps[f, rows(cell), :] - gap(cell - 1)
            if cell < 2:
                jump = jump + gap(cell)
            missing = linear_part(weights[cell], outside, cell)
            emit(f, cell, acc[f, rows(cell), :] - (missing + scaled[cell] * jump))


def exchange_kernel(
    ngx, ngz, cx, ny, state_ref, register_ref, ghost_ref, flags_ref,
    acc, xpad, mask, first_alpha, edge_flux, edge_near, jumps, done_register, done_state,
    zt, reg, ghost, flags, slots, mine, plane_top, acc_t, zf, zu, yf, yu, yq, zq, xf, near,
    load_sem, side_sem, send_sem, recv_sem, halo_send, halo_recv, ready_up, ready_wrap
):
    peers = Peers(ngx, ngz)
    gx, gz = peers.gx, peers.gz
    parts = ny // 8
    rows = cx * ny
    halo = 3 * ny
    strip = zt.shape[1] - 16
    chunk = strip // 8
    load = pltpu.make_async_copy(state_ref, xpad.at[:, pl.ds(halo, rows), :], load_sem)
    load.start()
    load_flags = pltpu.make_async_copy(flags_ref, flags, side_sem.at[0])
    load_ghost = pltpu.make_async_copy(ghost_ref, ghost, side_sem.at[1])
    load_register = pltpu.make_async_copy(register_ref, reg, load_sem)
    slots[...] = jnp.zeros(slots.shape, slots.dtype)
    barrier = pltpu.get_barrier_semaphore()
    peers.greet(barrier)
    load.wait()
    load_flags.start()
    load_ghost.start()
    load_register.start()
    best = None
    for row in range(0, rows, 8):
        cons = [xpad[var, pl.ds(halo + row, 8), :] for var in range(5)]
        inverse, vel, pressure = pressure_velocity(cons)
        sound = jnp.sqrt(GAMMA * pressure * inverse)
        local = [jnp.abs(v) + sound for v in vel]
        best = local if best is None else [jnp.maximum(a, b) for a, b in zip(best, local)]
    tops = [jnp.max(jnp.max(b, axis=0, keepdims=True), axis=1, keepdims=True) for b in best]
    lane = lax.broadcasted_iota(jnp.int32, (1, 128), 1)
    mine[...] = jnp.where(lane == 0, tops[0], jnp.where(lane == 1, tops[1], tops[2]))

    right, left = shifted(gx, 1, ngx), shifted(gx, ngx - 1, ngx)
    high, low = shifted(gz, 1, ngz), shifted(gz, ngz - 1, ngz)

    def move(leaves, comes, src, dst, target):
        return pltpu.make_async_remote_copy(
            src_ref=src, dst_ref=dst, send_sem=halo_send.at[leaves], recv_sem=halo_recv.at[comes],
            device_id=target, device_id_type=MESH,
        )

    def all_bytes(some, semaphore):
        pltpu.make_async_copy(some, some, semaphore).wait()

    blocks = xpad.reshape(5, cx + 6, ny, xpad.shape[2])
    to_left, to_right = [], []
    for part in range(parts):
        layers = lambda first: blocks.at[:, pl.ds(first, 3), pl.ds(part * 8, 8), :]
        to_left.append(move(1, 1, layers(3), layers(3 + cx), (left, gz)))
        to_right.append(move(1, 2 + part, layers(cx), layers(0), (right, gz)))

    def start(copies):
        for copy in copies:
            copy.start()

    def signal(semaphore, target):
        pl.semaphore_signal(semaphore, inc=1, device_id=target, device_id_type=MESH)

    def tell(source, far, index, target):
        pltpu.make_async_remote_copy(
            src_ref=source, dst_ref=slots.at[peers.q, index], send_sem=send_sem,
            recv_sem=recv_sem.at[far], device_id=target, device_id_type=MESH,
        ).start()

    pl.semaphore_wait(barrier, peers.greetings())

    def tell_lower(plane):
        @pl.when(plane < peers.q)
        def _():
            each(
                peers.members,
                lambda index: tell(mine, 1, peers.own, peers.member(plane, index)),
                peers.unroll,
            )

    each(peers.planes, tell_lower, peers.unroll)
    peers.plane_mates(lambda index, tx, tz: tell(mine, 0, peers.own, (tx, tz)))

    yields = peers.last & (gz > 0)

    @pl.when(peers.last)
    def _():
        signal(ready_wrap, (0, gz))
        start(to_right[:1])

    @pl.when(peers.last & (gz == 0))
    def _():
        start(to_right[1:])

    @pl.when((gx > 0) & jnp.logical_not(yields))
    def _():
        start(to_left)

    @pl.when(jnp.logical_not(peers.last))
    def _():
        start(to_right)

    peers.columns(lambda plane: plane < peers.q, lambda plane, target: signal(ready_up, target))
    for var in range(5):
        zt[var, pl.ds(8, strip), :] = xpad[var, pl.ds(halo, rows), :].T
    z_copies = [
        move(0, 0, zt.at[:, pl.ds(8, 8), :], zt.at[:, pl.ds(8 + strip, 8), :], (gx, low)),
        move(0, 0, zt.at[:, pl.ds(strip, 8), :], zt.at[:, pl.ds(0, 8), :], (gx, high)),
    ]
    start(z_copies)
    load_flags.wait()
    for x in range(cx):
        wide = jnp.broadcast_to(flags[x], (strip, ny)).astype(jnp.float32).T * (LAMBDA[0] / 12.0)
        mask[pl.ds(x * ny, ny), :] = wide
    mask_t = mask[...].T[:8]
    flag_t = mask_t > 0.0

    load_ghost.wait()
    for cell in range(ny + 6):
        y = cell - 3
        if y < ny:
            source = y if y >= 0 else -1 - y
            cons = [xpad[f, pl.ds(halo + source, 8, stride=ny), :] for f in range(5)]
            if y < 0:
                cons[2] = -cons[2]
        else:
            cons = [ghost[f, y - ny] for f in range(5)]
        store_fluxes(cons, 2, yf, yu, cell)
    load_register.wait()

    def y_linear(f, carry):
        for cell in range(ny):
            where = pl.ds(cell, 8, stride=ny)
            weights = difference_weights(mask[where, :] > 0.0)
            linear = linear_part(weights, lambda j: yf[f, j + 3], cell)
            acc[f, where, :] = REGISTER_DECAY * reg[f, where, :] - (LAMBDA[1] / 12.0) * linear
        prepare_line(ny, LAMBDA[1] / LAMBDA[0], f, yf, yu, yq)
        return carry

    lax.fori_loop(0, 5, y_linear, 0)

    @pl.when(yields)
    def _():
        start(to_right[1:])
        start(to_left)

    for part in range(parts):
        store_x_fluxes(ny, part, range(cx), xpad, xf)

    def x_prepare(f, part, centres, thirds):
        def keep(kind, j, value):
            near[part, kind, f, j - 1] = value

        flux = cached(lambda j: xf[part, f, j + 3])
        cons = cached(lambda j: xpad[f, pl.ds((j + 3) * ny + part * 8, 8), :])
        prepare(flux, cons, centres, keep)
        prepare_third(flux, cons, thirds, keep)

    def x_linear(f, part, cells, known):
        for cell in cells:
            where = pl.ds(cell * ny + part * 8, 8)
            weights = difference_weights(mask[where, :] > 0.0)
            linear = linear_part(weights, lambda j: xf[part, f, j + 3] if known(j) else None, cell)
            acc[f, where, :] = acc[f, where, :] - (LAMBDA[0] / 12.0) * linear

    def x_inner(f, carry):
        for part in range(parts):
            x_prepare(f, part, range(1, cx - 1), range(1, cx - 2))
            if part == parts - 1:
                for cell in range(5):
                    edge_flux[f, cell] = xf[part, f, cell + 3]
                for kind in range(11):
                    for j in range(1, 4):
                        edge_near[kind, f, j - 1] = near[part, kind, f, j - 1]
            x_linear(f, part, range(cx), lambda j: 0 <= j < cx)
        return carry

    lax.fori_loop(0, 5, x_inner, 0)

    def right_edge():
        all_bytes(xpad.at[:, pl.ds(0, halo), :], halo_recv.at[1])
        for part in range(parts):
            store_x_fluxes(ny, part, range(cx, cx + 3), xpad, xf)

        def field(f, carry):
            for part in range(parts):
                x_prepare(f, part, range(cx - 1, cx + 2), range(cx - 2, cx + 1))
                x_linear(f, part, range(cx - 3, cx), lambda j: j >= cx)
            return carry

        lax.fori_loop(0, 5, field, 0)

    all_bytes(zt.at[:, pl.ds(0, 16), :], halo_send.at[0])
    all_bytes(zt.at[:, pl.ds(0, 16), :], halo_recv.at[0])
    for cell in range(chunk + 6):
        cons = [zt[f, pl.ds(5 + cell, 8, stride=chunk), :] for f in range(5)]
        store_fluxes(cons, 3, zf, zu, cell)
    weights_t = [w * (-LAMBDA[2] / 12.0) for w in difference_weights(flag_t)]

    def z_linear(f, carry):
        for cell in range(chunk):
            linear = linear_part(weights_t, lambda j: zf[f, j + 3], cell)
            acc_t[f, pl.ds(cell, 8, stride=chunk), :] = linear
        acc[f] = acc[f] + acc_t[f].T
        prepare_line(chunk, LAMBDA[2] / LAMBDA[0], f, zf, zu, zq)
        return carry

    lax.fori_loop(0, 5, z_linear, 0)

    messages = slots.reshape(peers.planes * peers.members, 1, 128)

    def by_plane(count, semaphore):
        def visit(plane):
            number = count(plane)
            if number:
                @pl.when(peers.q == plane)
                def _():
                    all_bytes(messages.at[pl.ds(0, number)], semaphore)

        for plane in range(peers.planes):
            visit(plane)

    all_bytes(messages.at[pl.ds(0, peers.members - 1)], recv_sem.at[0])
    plane_top[...] = jnp.maximum(jnp.max(slots[peers.q], axis=0), mine[...])

    @pl.when(peers.q < peers.planes - 1)
    def _():
        pl.semaphore_wait(ready_up, peers.planes - 1 - peers.q)

    peers.columns(lambda plane: plane > peers.q, lambda plane, target: tell(plane_top, 1, 0, target))

    @pl.when(gx == 0)
    def _():
        pl.semaphore_wait(ready_wrap, 1)
        start(to_left)

    @pl.when(jnp.logical_not(peers.last))
    def _():
        right_edge()

    by_plane(lambda plane: (peers.planes - 1 - plane) * peers.members + plane, recv_sem.at[1])
    top = jnp.maximum(jnp.max(jnp.max(slots[...], axis=0), axis=0), mine[...])
    alpha = [jnp.broadcast_to(top[:, k : k + 1], (8, 128)) for k in range(3)]
    first_alpha[...] = alpha[0]

    def z_field(f, carry):
        gap = prepared_gaps(alpha[2], lambda k, j: zq[k, f, j + 2])
        before = gap(-1)
        for cell in range(chunk):
            after = gap(cell)
            acc_t[f, pl.ds(cell, 8, stride=chunk), :] = after - before
            before = after
        return carry

    lax.fori_loop(0, 5, z_field, 0, unroll=True)

    def y_field(f):
        gap = prepared_gaps(alpha[1], lambda k, j: yq[k, f, j + 2])
        before = gap(-1) if f == 2 else None
        for cell in range(ny):
            after = gap(cell)
            jumps[f, pl.ds(cell, 8, stride=ny), :] = after if before is None else after - before
            before = after

    for f in range(5):
        y_field(f)

    @pl.when(peers.last)
    def _():
        right_edge()

    def finish(part, f, cell, total):
        done_register[part, f, cell] = total
        state = xpad[f, pl.ds((cell + 3) * ny + part * 8, 8), :]
        done_state[part, f, cell] = state + UPDATE_WEIGHT * total

    def x_field(f, carry):
        turned = acc_t[f].T
        for part in range(parts):
            gap = prepared_gaps(alpha[0], lambda k, j: near[part, k, f, j - 1])
            for cell in range(cx):
                first = cell * ny + part * 8
                where = pl.ds(first, 8)
                jump = jumps[f, where, :] + turned[first : first + 8]
                if cell >= 2:
                    jump = jump + gap(cell)
                if cell >= 3:
                    finish(part, f, cell, acc[f, where, :] - mask[where, :] * (jump - gap(cell - 1)))
                else:
                    jumps[f, where, :] = jump
        return carry

    lax.fori_loop(0, 5, x_field, 0, unroll=True)

    for part in range(parts):
        if part == parts - 1:
            all_bytes(xpad.at[:, pl.ds(0, 2 * halo), :], halo_send.at[1])
            by_plane(lambda plane: (plane + 1) * peers.members - 1 + peers.planes - 1 - plane, send_sem)
        to_right[part].wait_recv()
        if part < parts - 1:
            store_x_fluxes(ny, part, range(-3, 0), xpad, xf)
            flux = lambda f, j: xf[part, f, j + 3]
            known = lambda k, f, j: near[part, k, f, j - 1]
            emit = functools.partial(finish, part)
            left_edge(ny, part, alpha[0], xpad, flux, mask, acc, known, jumps, emit)


def update_kernel(
    cx, ny, acc, xpad, mask, first_alpha, edge_flux, edge_near, jumps, done_register, done_state,
    state_out, register_out, late_register, late_state, sems
):
    last = ny // 8 - 1

    def put(src, dst, which):
        pltpu.make_async_copy(src, dst, sems.at[which]).start()

    for part in range(last + 1):
        first = 3 if part == last else 0
        block = pl.ds(first, cx - first)
        rows = pl.ds(part * 8, 8)
        put(done_register.at[part, :, block], register_out.at[:, block, rows, :], 0)
        put(done_state.at[part, :, block], state_out.at[:, block, rows, :], 1)
    halo = [
        fluxes_of([xpad[f, pl.ds((3 + cell) * ny + last * 8, 8), :] for f in range(5)], 1)
        for cell in range(-3, 0)
    ]

    def emit(f, cell, total):
        state = xpad[f, pl.ds((3 + cell) * ny + last * 8, 8), :]
        late_register[f, cell] = total
        late_state[f, cell] = state + UPDATE_WEIGHT * total

    alpha = first_alpha[...]
    flux = lambda f, j: halo[j + 3][f] if j < 0 else edge_flux[f, j]
    known = lambda k, f, j: edge_near[k, f, j - 1]
    left_edge(ny, last, alpha, xpad, flux, mask, acc, known, jumps, emit)
    block, rows = pl.ds(0, 3), pl.ds(last * 8, 8)
    put(late_register, register_out.at[:, block, rows, :], 0)
    put(late_state, state_out.at[:, block, rows, :], 1)
    for which, out in enumerate((register_out, state_out)):
        pltpu.make_async_copy(out, out, sems.at[which]).wait()


def shards(ngx, ngz, state, register, top_ghost, flags):
    _, cx, ny, cz = state.shape
    rows = cx * ny
    parts = ny // 8
    wide = plane_size(ngx)
    f32 = jnp.float32
    flat = lambda array: array.reshape(5, rows, cz)
    anywhere = pl.BlockSpec(memory_space=pl.ANY)
    inside = pl.BlockSpec(memory_space=pltpu.VMEM)
    held = pl.pallas_call(
        functools.partial(exchange_kernel, ngx, ngz, cx, ny),
        out_shape=(
            pltpu.VMEM((5, rows, cz), f32),
            pltpu.VMEM((5, (cx + 6) * ny, cz), f32),
            pltpu.VMEM((rows, cz), f32),
            pltpu.VMEM((8, 128), f32),
            pltpu.VMEM((5, 5, 8, cz), f32),
            pltpu.VMEM((11, 5, 3, 8, cz), f32),
            pltpu.VMEM((5, rows, cz), f32),
            pltpu.VMEM((parts, 5, cx, 8, cz), f32),
            pltpu.VMEM((parts, 5, cx, 8, cz), f32),
        ),
        in_specs=[anywhere] * 4,
        out_specs=(inside,) * 9,
        scratch_shapes=[
            pltpu.VMEM((5, cz + 16, rows), f32),
            pltpu.VMEM((5, rows, cz), f32),
            pltpu.VMEM((5, 3, cx, cz), f32),
            pltpu.VMEM((cx, 1, ny), jnp.int32),
            pltpu.VMEM((ngx // wide, wide * ngz, 1, 128), f32),
            pltpu.VMEM((1, 128), f32),
            pltpu.VMEM((1, 128), f32),
            pltpu.VMEM((5, cz, rows), f32),
            pltpu.VMEM((5, cz // 8 + 6, 8, rows), f32),
            pltpu.VMEM((5, cz // 8 + 6, 8, rows), f32),
            pltpu.VMEM((5, ny + 6, cx, cz), f32),
            pltpu.VMEM((5, ny + 6, cx, cz), f32),
            pltpu.VMEM((11, 5, ny + 4, cx, cz), f32),
            pltpu.VMEM((11, 5, cz // 8 + 4, 8, rows), f32),
            pltpu.VMEM((parts, 5, cx + 6, 8, cz), f32),
            pltpu.VMEM((parts, 11, 5, cx + 1, 8, cz), f32),
            pltpu.SemaphoreType.DMA,
            pltpu.SemaphoreType.DMA((2,)),
            pltpu.SemaphoreType.DMA,
            pltpu.SemaphoreType.DMA((2,)),
            pltpu.SemaphoreType.DMA((2,)),
            pltpu.SemaphoreType.DMA((2 + parts,)),
            pltpu.SemaphoreType.REGULAR,
            pltpu.SemaphoreType.REGULAR,
        ],
        compiler_params=pltpu.CompilerParams(collective_id=0, has_side_effects=True),
        name="exchange",
    )(flat(state), flat(register), top_ghost.transpose(0, 2, 1, 3), flags.transpose(0, 2, 1))
    block = jax.ShapeDtypeStruct(state.shape, f32)
    return pl.pallas_call(
        functools.partial(update_kernel, cx, ny),
        out_shape=(block, block),
        in_specs=[inside] * 9,
        out_specs=(anywhere, anywhere),
        scratch_shapes=[
            pltpu.VMEM((5, 3, 8, cz), f32),
            pltpu.VMEM((5, 3, 8, cz), f32),
            pltpu.SemaphoreType.DMA((2,)),
        ],
        name="update",
    )(*(pltpu.with_memory_space_constraint(array, pltpu.VMEM) for array in held))


def solution(mesh):
    block = P(None, "gx", None, "gz")
    return jax.shard_map(
        functools.partial(shards, mesh.shape["gx"], mesh.shape["gz"]),
        mesh=mesh,
        in_specs=(block, block, block, P("gx", None, "gz")),
        out_specs=(block, block),
        check_vma=False,
    )
```

```python
import functools

import jax
import jax.numpy as jnp
from jax import lax
from jax.experimental import pallas as pl
from jax.experimental.pallas import tpu as pltpu
from jax.sharding import PartitionSpec as P

MESH = pl.DeviceIdType.MESH
GAMMA = 1.4
EPS_WENO = 1e-06
LAMBDA = (0.1, 0.15, 0.1)
REGISTER_DECAY = -5.0 / 9.0
UPDATE_WEIGHT = 15.0 / 16.0
UNROLL_LIMIT = 64
MID = 6.0**-0.5


def reciprocal(value):
    return pltpu.reciprocal(value, approx=False)


def pressure_velocity(cons):
    inverse = reciprocal(cons[0])
    vel = [cons[1] * inverse, cons[2] * inverse, cons[3] * inverse]
    pressure = (GAMMA - 1.0) * (
        cons[4] - 0.5 * (cons[1] * vel[0] + cons[2] * vel[1] + cons[3] * vel[2])
    )
    return inverse, vel, pressure


def shifted(me, step, count):
    moved = me + step
    return jnp.where(moved >= count, moved - count, moved)


def each(count, action, unroll):
    if unroll:
        for index in range(count):
            action(index)
    else:
        def body(index, carry):
            action(index)
            return carry
        lax.fori_loop(0, count, body, 0)


def plane_size(ngx):
    return max(p for p in range(1, ngx + 1) if ngx % p == 0 and p * p <= ngx)


class Peers:
    def __init__(self, ngx, ngz):
        self.ngx, self.ngz = ngx, ngz
        self.gx, self.gz = lax.axis_index("gx"), lax.axis_index("gz")
        self.wide = plane_size(ngx)
        self.planes = ngx // self.wide
        self.members = self.wide * ngz
        self.q, self.r = lax.div(self.gx, self.wide), lax.rem(self.gx, self.wide)
        self.own = self.r * ngz + self.gz
        self.last = self.gx == ngx - 1
        self.unroll = self.planes * self.members < UNROLL_LIMIT

    def member(self, plane, index):
        if isinstance(index, int):
            return plane * self.wide + index // self.ngz, index % self.ngz
        return plane * self.wide + lax.div(index, self.ngz), lax.rem(index, self.ngz)

    def plane_mates(self, action):
        def visit(index):
            @pl.when(self.own != index)
            def _():
                action(index, *self.member(self.q, index))
        each(self.members, visit, self.unroll)

    def of_planes(self, wanted, action):
        def visit(plane):
            @pl.when(wanted(plane))
            def _():
                each(self.members, lambda index: action(index, *self.member(plane, index)), self.unroll)
        each(self.planes, visit, self.unroll)

    def columns(self, wanted, action):
        def visit(plane):
            @pl.when(wanted(plane))
            def _():
                action(plane, (plane * self.wide + self.r, self.gz))
        each(self.planes, visit, self.unroll)

    def greet(self, barrier):
        def signal(tx, tz):
            pl.semaphore_signal(barrier, inc=1, device_id=(tx, tz), device_id_type=MESH)

        @pl.when((self.r == 0) & (self.gx > 0))
        def _():
            signal(self.gx - 1, self.gz)

        self.plane_mates(lambda index, tx, tz: signal(tx, tz))
        self.of_planes(lambda plane: plane > self.q, lambda index, tx, tz: signal(tx, tz))

    def greetings(self):
        has_next = (self.r == self.wide - 1) & jnp.logical_not(self.last)
        return self.members - 1 + self.q * self.members + has_next.astype(jnp.int32)


def cached(function):
    return functools.lru_cache(None)(function)


class Line:
    def __init__(self, load):
        self.load = cached(load)
        self.D = cached(lambda j: self.load(j + 1) - self.load(j))
        self.S = cached(lambda j: self.D(j) - self.D(j - 1))
        self.T = cached(lambda j: self.S(j + 1) - self.S(j))
        self.S2 = cached(lambda j: self.S(j) + self.S(j))
        self.C = cached(
            lambda j: (self.S(j) * self.S(j) * (4.0 / 3.0) + 4.0 * EPS_WENO)
            + self.D(j) * self.D(j - 1)
        )
        self.L = cached(lambda j: self.C(j) + self.S2(j) * self.D(j))
        self.M = cached(lambda j: MID * self.C(j))
        self.R = cached(lambda j: self.C(j) - self.S2(j) * self.D(j - 1))


def correction(near, mid, far, t_near, t_far):
    a, b, c = mid * far, near * far, near * mid
    w_near = a * a
    w_far = 3.0 * (c * c)
    total = w_near + b * b + w_far
    return (w_far * t_far + (w_near + w_near) * t_near) * reciprocal(total)


def face_gap(plus, minus, drift_t):
    def gap(j):
        up = correction(plus.L(j - 1), plus.M(j), plus.R(j + 1), plus.T(j - 1), plus.T(j))
        down = correction(minus.R(j + 2), minus.M(j + 1), minus.L(j), minus.T(j + 1), minus.T(j))
        return drift_t(j) - up + down

    return gap


KINDS = ("L", "M", "R")


def prepare(flux, cons, cells, store):
    f, u = Line(flux), Line(cons)
    for j in cells:
        mixed = (8.0 / 3.0) * (f.S(j) * u.S(j)) + (f.D(j) * u.D(j - 1) + f.D(j - 1) * u.D(j))
        curved = (4.0 / 3.0) * (u.S(j) * u.S(j)) + u.D(j) * u.D(j - 1)
        centre = (f.C(j), mixed, curved)

        def product(at):
            return (
                f.S2(j) * f.D(at),
                f.S2(j) * u.D(at) + u.S2(j) * f.D(at),
                u.S2(j) * u.D(at),
            )

        left = [c + p for c, p in zip(centre, product(j))]
        right = [c - p for c, p in zip(centre, product(j - 1))]
        for kind, terms in enumerate((left, [MID * c for c in centre], right)):
            for power, term in enumerate(terms):
                store(3 * kind + power, j, term)


def prepare_third(flux, cons, cells, store, scale=1.0):
    f, u = Line(flux), Line(cons)
    for j in cells:
        store(9, j, f.T(j) if scale == 1.0 else scale * f.T(j))
        store(10, j, u.T(j) if scale == 1.0 else scale * u.T(j))


class Prepared:
    def __init__(self, alpha, load):
        square = alpha * alpha

        def both(kind):
            def pair(j):
                even = load(3 * kind, j) + square * load(3 * kind + 2, j)
                odd = alpha * load(3 * kind + 1, j)
                return even + odd, even - odd
            return cached(pair)

        self.drift_t = cached(lambda j: alpha * load(10, j))
        third = cached(lambda j: (load(9, j) + self.drift_t(j), load(9, j) - self.drift_t(j)))
        pairs = {name: both(kind) for kind, name in enumerate(KINDS)} | {"T": third}
        self.side = [
            {name: (lambda j, pair=pair, k=k: pair(j)[k]) for name, pair in pairs.items()} for k in range(2)
        ]


class Side:
    def __init__(self, values):
        self.L, self.M, self.R, self.T = (values[name] for name in (*KINDS, "T"))


def prepared_gaps(alpha, load):
    ready = Prepared(alpha, load)
    return face_gap(Side(ready.side[0]), Side(ready.side[1]), ready.drift_t)


def edge_gaps(alpha, load_flux, load_cons, load, inner, inner_t):
    flux = cached(load_flux)
    drift = cached(lambda j: alpha * load_cons(j))
    ready = Prepared(alpha, load)
    fresh = Line(lambda j: flux(j) + drift(j)), Line(lambda j: flux(j) - drift(j))

    def mixed(k):
        def pick(name):
            known = inner_t if name == "T" else inner
            return lambda j: ready.side[k][name](j) if j in known else getattr(fresh[k], name)(j)
        return Side({name: pick(name) for name in (*KINDS, "T")})

    plus, minus = mixed(0), mixed(1)

    def drift_t(j):
        return ready.drift_t(j) if j in inner_t else 0.5 * (plus.T(j) - minus.T(j))

    return face_gap(plus, minus, drift_t)


def difference_weights(flagged):
    return (
        jnp.where(flagged, 8.0, 9.0),
        jnp.where(flagged, -1.0, -1.8),
        jnp.where(flagged, 0.0, 0.2),
    )


def linear_part(weights, flux, cell):
    total = None
    for reach, weight in enumerate(weights, 1):
        high, low = flux(cell + reach), flux(cell - reach)
        if high is None and low is None:
            continue
        gap = -low if high is None else high if low is None else high - low
        total = weight * gap if total is None else total + weight * gap
    return total


def fluxes_of(cons, var):
    _, vel, pressure = pressure_velocity(cons)
    velocity = vel[var - 1]
    fluxes = [cons[field] * velocity for field in range(4)]
    fluxes.append((cons[4] + pressure) * velocity)
    fluxes[var] = fluxes[var] + pressure
    return fluxes


def store_fluxes(cons, var, fluxes, conserved, cell):
    for field, flux in enumerate(fluxes_of(cons, var)):
        fluxes[field, cell] = flux
        conserved[field, cell] = cons[field]


def prepare_line(count, scale, f, fluxes, conserved, out):
    def keep(kind, j, value):
        out[kind, f, j + 2] = value

    flux, cons = cached(lambda j: fluxes[f, j + 3]), cached(lambda j: conserved[f, j + 3])
    prepare(flux, cons, range(-2, count + 2), keep)
    prepare_third(flux, cons, range(-2, count + 1), keep, scale)


def store_x_fluxes(ny, part, cells, xpad, xf):
    for cell in cells:
        cons = [xpad[f, pl.ds((cell + 3) * ny + part * 8, 8), :] for f in range(5)]
        for field, flux in enumerate(fluxes_of(cons, 1)):
            xf[part, field, cell + 3] = flux


def left_edge(ny, part, alpha, xpad, flux, mask, acc, known, jumps, emit):
    rows = lambda cell: pl.ds(cell * ny + part * 8, 8)
    scaled = [mask[rows(cell), :] for cell in range(3)]
    weights = [
        [weight * (LAMBDA[0] / 12.0) for weight in difference_weights(m > 0.0)] for m in scaled
    ]
    for f in range(5):
        gap = edge_gaps(
            alpha, lambda j: flux(f, j), lambda j: xpad[f, rows(j + 3), :],
            lambda k, j: known(k, f, j), range(1, 4), range(1, 4),
        )
        outside = lambda j: flux(f, j) if j < 0 else None
        for cell in range(3):
            jump = jumps[f, rows(cell), :] - gap(cell - 1)
            if cell < 2:
                jump = jump + gap(cell)
            missing = linear_part(weights[cell], outside, cell)
            emit(f, cell, acc[f, rows(cell), :] - (missing + scaled[cell] * jump))


def exchange_kernel(
    ngx, ngz, cx, ny, state_ref, register_ref, ghost_ref, flags_ref,
    acc, xpad, mask, first_alpha, edge_flux, edge_near, jumps, done_register, done_state,
    zt, reg, ghost, flags, slots, mine, plane_top, acc_t, zf, zu, yf, yu, yq, zq, xf, near,
    load_sem, side_sem, send_sem, recv_sem, halo_send, halo_recv, ready_up, ready_wrap
):
    peers = Peers(ngx, ngz)
    gx, gz = peers.gx, peers.gz
    parts = ny // 8
    rows = cx * ny
    halo = 3 * ny
    strip = zt.shape[1] - 16
    chunk = strip // 8
    half = rows // 2
    loads = [
        pltpu.make_async_copy(
            state_ref.at[:, pl.ds(first, half), :], xpad.at[:, pl.ds(halo + first, half), :], load_sem.at[k]
        )
        for k, first in enumerate((0, half))
    ]
    for load in loads:
        load.start()
    load_flags = pltpu.make_async_copy(flags_ref, flags, side_sem.at[0])
    load_ghost = pltpu.make_async_copy(ghost_ref, ghost, side_sem.at[1])
    load_register = pltpu.make_async_copy(register_ref, reg, load_sem.at[0])
    slots[...] = jnp.zeros(slots.shape, slots.dtype)
    barrier = pltpu.get_barrier_semaphore()
    peers.greet(barrier)
    best = None
    for row in range(0, rows, 8):
        if row % half == 0:
            loads[row // half].wait()
        cons = [xpad[var, pl.ds(halo + row, 8), :] for var in range(5)]
        inverse, vel, pressure = pressure_velocity(cons)
        sound = jnp.sqrt(GAMMA * pressure * inverse)
        local = [jnp.abs(v) + sound for v in vel]
        best = local if best is None else [jnp.maximum(a, b) for a, b in zip(best, local)]
    tops = [jnp.max(jnp.max(b, axis=0, keepdims=True), axis=1, keepdims=True) for b in best]
    lane = lax.broadcasted_iota(jnp.int32, (1, 128), 1)
    load_flags.start()
    load_ghost.start()
    load_register.start()
    mine[...] = jnp.where(lane == 0, tops[0], jnp.where(lane == 1, tops[1], tops[2]))

    right, left = shifted(gx, 1, ngx), shifted(gx, ngx - 1, ngx)
    high, low = shifted(gz, 1, ngz), shifted(gz, ngz - 1, ngz)

    def move(leaves, comes, src, dst, target):
        return pltpu.make_async_remote_copy(
            src_ref=src, dst_ref=dst, send_sem=halo_send.at[leaves], recv_sem=halo_recv.at[comes],
            device_id=target, device_id_type=MESH,
        )

    def all_bytes(some, semaphore):
        pltpu.make_async_copy(some, some, semaphore).wait()

    blocks = xpad.reshape(5, cx + 6, ny, xpad.shape[2])
    to_left, to_right = [], []
    for part in range(parts):
        layers = lambda first: blocks.at[:, pl.ds(first, 3), pl.ds(part * 8, 8), :]
        to_left.append(move(1, 1, layers(3), layers(3 + cx), (left, gz)))
        to_right.append(move(1, 2 + part, layers(cx), layers(0), (right, gz)))

    def start(copies):
        for copy in copies:
            copy.start()

    def signal(semaphore, target):
        pl.semaphore_signal(semaphore, inc=1, device_id=target, device_id_type=MESH)

    def tell(source, far, index, target):
        pltpu.make_async_remote_copy(
            src_ref=source, dst_ref=slots.at[peers.q, index], send_sem=send_sem,
            recv_sem=recv_sem.at[far], device_id=target, device_id_type=MESH,
        ).start()

    pl.semaphore_wait(barrier, peers.greetings())

    def tell_lower(plane):
        @pl.when(plane < peers.q)
        def _():
            each(
                peers.members,
                lambda index: tell(mine, 1, peers.own, peers.member(plane, index)),
                peers.unroll,
            )

    each(peers.planes, tell_lower, peers.unroll)
    peers.plane_mates(lambda index, tx, tz: tell(mine, 0, peers.own, (tx, tz)))

    yields = peers.last & (gz > 0)

    @pl.when(peers.last)
    def _():
        signal(ready_wrap, (0, gz))
        start(to_right[:1])

    @pl.when(peers.last & (gz == 0))
    def _():
        start(to_right[1:])

    @pl.when((gx > 0) & jnp.logical_not(yields))
    def _():
        start(to_left)

    @pl.when(jnp.logical_not(peers.last))
    def _():
        start(to_right)

    peers.columns(lambda plane: plane < peers.q, lambda plane, target: signal(ready_up, target))
    for var in range(5):
        zt[var, pl.ds(8, strip), :] = xpad[var, pl.ds(halo, rows), :].T
    z_copies = [
        move(0, 0, zt.at[:, pl.ds(8, 8), :], zt.at[:, pl.ds(8 + strip, 8), :], (gx, low)),
        move(0, 0, zt.at[:, pl.ds(strip, 8), :], zt.at[:, pl.ds(0, 8), :], (gx, high)),
    ]
    start(z_copies)
    load_flags.wait()
    for x in range(cx):
        wide = jnp.broadcast_to(flags[x], (strip, ny)).astype(jnp.float32).T * (LAMBDA[0] / 12.0)
        mask[pl.ds(x * ny, ny), :] = wide
    mask_t = mask[...].T[:8]
    flag_t = mask_t > 0.0

    load_ghost.wait()
    for cell in range(ny + 6):
        y = cell - 3
        if y < ny:
            source = y if y >= 0 else -1 - y
            cons = [xpad[f, pl.ds(halo + source, 8, stride=ny), :] for f in range(5)]
            if y < 0:
                cons[2] = -cons[2]
        else:
            cons = [ghost[f, y - ny] for f in range(5)]
        store_fluxes(cons, 2, yf, yu, cell)
    load_register.wait()

    def y_linear(f, carry):
        for cell in range(ny):
            where = pl.ds(cell, 8, stride=ny)
            weights = difference_weights(mask[where, :] > 0.0)
            linear = linear_part(weights, lambda j: yf[f, j + 3], cell)
            acc[f, where, :] = REGISTER_DECAY * reg[f, where, :] - (LAMBDA[1] / 12.0) * linear
        prepare_line(ny, LAMBDA[1] / LAMBDA[0], f, yf, yu, yq)
        return carry

    lax.fori_loop(0, 5, y_linear, 0)

    @pl.when(yields)
    def _():
        start(to_right[1:])
        start(to_left)

    for part in range(parts):
        store_x_fluxes(ny, part, range(cx), xpad, xf)

    def x_prepare(f, part, centres, thirds):
        def keep(kind, j, value):
            near[part, kind, f, j - 1] = value

        flux = cached(lambda j: xf[part, f, j + 3])
        cons = cached(lambda j: xpad[f, pl.ds((j + 3) * ny + part * 8, 8), :])
        prepare(flux, cons, centres, keep)
        prepare_third(flux, cons, thirds, keep)

    def x_linear(f, part, cells, known):
        for cell in cells:
            where = pl.ds(cell * ny + part * 8, 8)
            weights = difference_weights(mask[where, :] > 0.0)
            linear = linear_part(weights, lambda j: xf[part, f, j + 3] if known(j) else None, cell)
            acc[f, where, :] = acc[f, where, :] - (LAMBDA[0] / 12.0) * linear

    def x_inner(f, carry):
        for part in range(parts):
            x_prepare(f, part, range(1, cx - 1), range(1, cx - 2))
            if part == parts - 1:
                for cell in range(5):
                    edge_flux[f, cell] = xf[part, f, cell + 3]
                for kind in range(11):
                    for j in range(1, 4):
                        edge_near[kind, f, j - 1] = near[part, kind, f, j - 1]
            x_linear(f, part, range(cx), lambda j: 0 <= j < cx)
        return carry

    lax.fori_loop(0, 5, x_inner, 0)

    def right_edge():
        all_bytes(xpad.at[:, pl.ds(0, halo), :], halo_recv.at[1])
        for part in range(parts):
            store_x_fluxes(ny, part, range(cx, cx + 3), xpad, xf)

        def field(f, carry):
            for part in range(parts):
                x_prepare(f, part, range(cx - 1, cx + 2), range(cx - 2, cx + 1))
                x_linear(f, part, range(cx - 3, cx), lambda j: j >= cx)
            return carry

        lax.fori_loop(0, 5, field, 0)

    all_bytes(zt.at[:, pl.ds(0, 16), :], halo_send.at[0])
    all_bytes(zt.at[:, pl.ds(0, 16), :], halo_recv.at[0])
    for cell in range(chunk + 6):
        cons = [zt[f, pl.ds(5 + cell, 8, stride=chunk), :] for f in range(5)]
        store_fluxes(cons, 3, zf, zu, cell)
    weights_t = [w * (-LAMBDA[2] / 12.0) for w in difference_weights(flag_t)]

    def z_linear(f, carry):
        for cell in range(chunk):
            linear = linear_part(weights_t, lambda j: zf[f, j + 3], cell)
            acc_t[f, pl.ds(cell, 8, stride=chunk), :] = linear
        acc[f] = acc[f] + acc_t[f].T
        prepare_line(chunk, LAMBDA[2] / LAMBDA[0], f, zf, zu, zq)
        return carry

    lax.fori_loop(0, 5, z_linear, 0)

    messages = slots.reshape(peers.planes * peers.members, 1, 128)

    def by_plane(count, semaphore):
        def visit(plane):
            number = count(plane)
            if number:
                @pl.when(peers.q == plane)
                def _():
                    all_bytes(messages.at[pl.ds(0, number)], semaphore)

        for plane in range(peers.planes):
            visit(plane)

    all_bytes(messages.at[pl.ds(0, peers.members - 1)], recv_sem.at[0])
    plane_top[...] = jnp.maximum(jnp.max(slots[peers.q], axis=0), mine[...])

    @pl.when(peers.q < peers.planes - 1)
    def _():
        pl.semaphore_wait(ready_up, peers.planes - 1 - peers.q)

    peers.columns(lambda plane: plane > peers.q, lambda plane, target: tell(plane_top, 1, 0, target))

    @pl.when(gx == 0)
    def _():
        pl.semaphore_wait(ready_wrap, 1)
        start(to_left)

    @pl.when(jnp.logical_not(peers.last))
    def _():
        right_edge()

    by_plane(lambda plane: (peers.planes - 1 - plane) * peers.members + plane, recv_sem.at[1])
    top = jnp.maximum(jnp.max(jnp.max(slots[...], axis=0), axis=0), mine[...])
    alpha = [jnp.broadcast_to(top[:, k : k + 1], (8, 128)) for k in range(3)]
    first_alpha[...] = alpha[0]

    def z_field(f, carry):
        gap = prepared_gaps(alpha[2], lambda k, j: zq[k, f, j + 2])
        before = gap(-1)
        for cell in range(chunk):
            after = gap(cell)
            acc_t[f, pl.ds(cell, 8, stride=chunk), :] = after - before
            before = after
        return carry

    lax.fori_loop(0, 5, z_field, 0, unroll=True)

    def y_field(f):
        gap = prepared_gaps(alpha[1], lambda k, j: yq[k, f, j + 2])
        before = gap(-1) if f == 2 else None
        for cell in range(ny):
            after = gap(cell)
            jumps[f, pl.ds(cell, 8, stride=ny), :] = after if before is None else after - before
            before = after

    for f in range(5):
        y_field(f)

    @pl.when(peers.last)
    def _():
        right_edge()

    def finish(part, f, cell, total):
        done_register[part, f, cell] = total
        state = xpad[f, pl.ds((cell + 3) * ny + part * 8, 8), :]
        done_state[part, f, cell] = state + UPDATE_WEIGHT * total

    def x_field(f, carry):
        turned = acc_t[f].T
        for part in range(parts):
            gap = prepared_gaps(alpha[0], lambda k, j: near[part, k, f, j - 1])
            for cell in range(cx):
                first = cell * ny + part * 8
                where = pl.ds(first, 8)
                jump = jumps[f, where, :] + turned[first : first + 8]
                if cell >= 2:
                    jump = jump + gap(cell)
                if cell >= 3:
                    finish(part, f, cell, acc[f, where, :] - mask[where, :] * (jump - gap(cell - 1)))
                else:
                    jumps[f, where, :] = jump
        return carry

    lax.fori_loop(0, 5, x_field, 0, unroll=True)

    for part in range(parts):
        if part == parts - 1:
            all_bytes(xpad.at[:, pl.ds(0, 2 * halo), :], halo_send.at[1])
            by_plane(lambda plane: (plane + 1) * peers.members - 1 + peers.planes - 1 - plane, send_sem)
        to_right[part].wait_recv()
        if part < parts - 1:
            store_x_fluxes(ny, part, range(-3, 0), xpad, xf)
            flux = lambda f, j: xf[part, f, j + 3]
            known = lambda k, f, j: near[part, k, f, j - 1]
            emit = functools.partial(finish, part)
            left_edge(ny, part, alpha[0], xpad, flux, mask, acc, known, jumps, emit)


def update_kernel(
    cx, ny, acc, xpad, mask, first_alpha, edge_flux, edge_near, jumps, done_register, done_state,
    state_out, register_out, late_register, late_state, sems
):
    last = ny // 8 - 1

    def put(src, dst, which):
        pltpu.make_async_copy(src, dst, sems.at[which]).start()

    for part in range(last + 1):
        first = 3 if part == last else 0
        block = pl.ds(first, cx - first)
        rows = pl.ds(part * 8, 8)
        put(done_register.at[part, :, block], register_out.at[:, block, rows, :], 0)
        put(done_state.at[part, :, block], state_out.at[:, block, rows, :], 1)
    halo = [
        fluxes_of([xpad[f, pl.ds((3 + cell) * ny + last * 8, 8), :] for f in range(5)], 1)
        for cell in range(-3, 0)
    ]

    def emit(f, cell, total):
        state = xpad[f, pl.ds((3 + cell) * ny + last * 8, 8), :]
        late_register[f, cell] = total
        late_state[f, cell] = state + UPDATE_WEIGHT * total

    alpha = first_alpha[...]
    flux = lambda f, j: halo[j + 3][f] if j < 0 else edge_flux[f, j]
    known = lambda k, f, j: edge_near[k, f, j - 1]
    left_edge(ny, last, alpha, xpad, flux, mask, acc, known, jumps, emit)
    block, rows = pl.ds(0, 3), pl.ds(last * 8, 8)
    put(late_register, register_out.at[:, block, rows, :], 0)
    put(late_state, state_out.at[:, block, rows, :], 1)
    for which, out in enumerate((register_out, state_out)):
        pltpu.make_async_copy(out, out, sems.at[which]).wait()


def shards(ngx, ngz, state, register, top_ghost, flags):
    _, cx, ny, cz = state.shape
    rows = cx * ny
    parts = ny // 8
    wide = plane_size(ngx)
    f32 = jnp.float32
    flat = lambda array: array.reshape(5, rows, cz)
    anywhere = pl.BlockSpec(memory_space=pl.ANY)
    inside = pl.BlockSpec(memory_space=pltpu.VMEM)
    held = pl.pallas_call(
        functools.partial(exchange_kernel, ngx, ngz, cx, ny),
        out_shape=(
            pltpu.VMEM((5, rows, cz), f32),
            pltpu.VMEM((5, (cx + 6) * ny, cz), f32),
            pltpu.VMEM((rows, cz), f32),
            pltpu.VMEM((8, 128), f32),
            pltpu.VMEM((5, 5, 8, cz), f32),
            pltpu.VMEM((11, 5, 3, 8, cz), f32),
            pltpu.VMEM((5, rows, cz), f32),
            pltpu.VMEM((parts, 5, cx, 8, cz), f32),
            pltpu.VMEM((parts, 5, cx, 8, cz), f32),
        ),
        in_specs=[anywhere] * 4,
        out_specs=(inside,) * 9,
        scratch_shapes=[
            pltpu.VMEM((5, cz + 16, rows), f32),
            pltpu.VMEM((5, rows, cz), f32),
            pltpu.VMEM((5, 3, cx, cz), f32),
            pltpu.VMEM((cx, 1, ny), jnp.int32),
            pltpu.VMEM((ngx // wide, wide * ngz, 1, 128), f32),
            pltpu.VMEM((1, 128), f32),
            pltpu.VMEM((1, 128), f32),
            pltpu.VMEM((5, cz, rows), f32),
            pltpu.VMEM((5, cz // 8 + 6, 8, rows), f32),
            pltpu.VMEM((5, cz // 8 + 6, 8, rows), f32),
            pltpu.VMEM((5, ny + 6, cx, cz), f32),
            pltpu.VMEM((5, ny + 6, cx, cz), f32),
            pltpu.VMEM((11, 5, ny + 4, cx, cz), f32),
            pltpu.VMEM((11, 5, cz // 8 + 4, 8, rows), f32),
            pltpu.VMEM((parts, 5, cx + 6, 8, cz), f32),
            pltpu.VMEM((parts, 11, 5, cx + 1, 8, cz), f32),
            pltpu.SemaphoreType.DMA((2,)),
            pltpu.SemaphoreType.DMA((2,)),
            pltpu.SemaphoreType.DMA,
            pltpu.SemaphoreType.DMA((2,)),
            pltpu.SemaphoreType.DMA((2,)),
            pltpu.SemaphoreType.DMA((2 + parts,)),
            pltpu.SemaphoreType.REGULAR,
            pltpu.SemaphoreType.REGULAR,
        ],
        compiler_params=pltpu.CompilerParams(collective_id=0, has_side_effects=True),
        name="exchange",
    )(flat(state), flat(register), top_ghost.transpose(0, 2, 1, 3), flags.transpose(0, 2, 1))
    block = jax.ShapeDtypeStruct(state.shape, f32)
    return pl.pallas_call(
        functools.partial(update_kernel, cx, ny),
        out_shape=(block, block),
        in_specs=[inside] * 9,
        out_specs=(anywhere, anywhere),
        scratch_shapes=[
            pltpu.VMEM((5, 3, 8, cz), f32),
            pltpu.VMEM((5, 3, 8, cz), f32),
            pltpu.SemaphoreType.DMA((2,)),
        ],
        name="update",
    )(*(pltpu.with_memory_space_constraint(array, pltpu.VMEM) for array in held))


def solution(mesh):
    block = P(None, "gx", None, "gz")
    return jax.shard_map(
        functools.partial(shards, mesh.shape["gx"], mesh.shape["gz"]),
        mesh=mesh,
        in_specs=(block, block, block, P("gx", None, "gz")),
        out_specs=(block, block),
        check_vma=False,
    )
```
